128 devices in a mesh: narrow: 2 (over core), wide: 64 (over x, y, z).
Axes of the slice: x: 4, y: 4, z: 4, core: 2. Of those that a mesh axis runs over, the one named last changes fastest.
Arguments:
- embeddings: bfloat16 [32768, 256], P(('narrow', 'wide')), may hold values from -6 to 6
- noise: float32 [32768], P(('narrow', 'wide')), may hold values from 0.05 to 0.5
- targets: float32 [32768, 64], P(('narrow', 'wide')), may hold values from -6 to 6
- level_scale: float32 [7], replicated, may hold values from 1.5 to 4
- skeleton: int32 [7, 128, 256], P(None, ('narrow', 'wide')), may hold values from 0 to 32767, as said below
Outputs:
- solution: float32 [32768, 64], P(('narrow', 'wide'))
- fit: float32 [64], replicated
- logdet: float32 [], replicated
The draws below stay inside these ranges and needn't reach their ends.
Inputs may be any that keep to these rules, and one draw needn't show every extreme that they name: `skeleton`: for each level l (first index l - 1), all devices whose index in narrow+wide has the same quotient by 2**l hold equal rows, and each row holds 256 distinct indices of points of that level-l node.
All inputs are finite; a program needn't handle non-finite values.
Results may differ from the reference program's by a relative error of at most 0.0003.
Values may be sent and summed in bfloat16 or wider, within the bound.
A program may use at most 128 MiB of HBM per device.

```python
import math
import jax
import jax.numpy as jnp
from jax import lax

WIDTH = 256
RANK = 256
RHS = 64
LEAF = 256
LEVELS = 7
NPTS = 32768
DEVICES = 128


def draw_embeddings(key, part):
    npoints = LEAF * DEVICES
    clusters = max(RANK // 8, 2)
    center_key = jax.random.fold_in(key, 101)
    member_key = jax.random.fold_in(key, 202)
    spread_key = jax.random.fold_in(key, 303)
    centers = 0.85 * jax.random.normal(center_key, (clusters, WIDTH), jnp.float32)
    member = jax.random.randint(member_key, (npoints,), 0, clusters)
    spread = 0.53 * jax.random.normal(spread_key, (npoints, WIDTH), jnp.float32)
    values = jnp.take(centers, member, axis=0) + spread
    return jnp.clip(values, -6.0, 6.0).astype(jnp.bfloat16)


def draw_skeleton(key, part):
    npoints = LEAF * DEVICES
    stacked = []
    for level in range(1, LEVELS + 1):
        span = LEAF * 2 ** level
        nodes = npoints // span
        level_key = jax.random.fold_in(key, 7919 + level)
        scores = jax.random.randint(level_key, (nodes, span), 0, 2 ** 30 // span) * span
        scores = scores + jnp.arange(span, dtype=jnp.int32)[None, :]
        _, picked = lax.top_k(scores, RANK)
        picked = picked + (jnp.arange(nodes, dtype=jnp.int32) * span)[:, None]
        stacked.append(jnp.repeat(picked, 2 ** level, axis=0))
    return jnp.stack(stacked).astype(jnp.int32)


def block_scale(rng, extent, cuts, low, top_value):
    gain = 1.0
    for axis_at, blocks in cuts:
        steps = jax.random.uniform(jax.random.fold_in(jax.random.fold_in(rng, 6), axis_at), (blocks,), jnp.float32, low / len(cuts), top_value / len(cuts))
        gain = gain * jnp.repeat(jnp.exp(steps), extent[axis_at] // blocks).reshape((-1,) + (1,) * (len(extent) - 1 - axis_at))
    return gain


def gaussian(own_key, extent, deviation, reach, split=(), held_as=jnp.bfloat16):
    values = jax.random.normal(own_key, extent, jnp.float32) * deviation
    if len(split) > 0:
        values = block_scale(own_key, extent, split, -0.22, 0.18) * values
    return jnp.clip(values, min=-reach, max=reach).astype(held_as)


def setup_inputs(seed: int = 0) -> dict:
    key_of = jax.random.split(jax.random.key(seed), 6)
    embeddings = draw_embeddings(jax.random.fold_in(key_of[5], 71), 0)
    noise = jnp.clip(jnp.exp(math.log(0.5) - 2.3025851 * jax.random.uniform(key_of[1], (NPTS,), jnp.float32) ** block_scale(key_of[1], (NPTS,), ((0, 128),), -0.2, 0.2)), 0.05, 0.5)
    targets = gaussian(key_of[2], (NPTS, RHS), 1.0, 6.0, ((0, 128),), jnp.float32)
    level_scale = jnp.clip(jnp.exp(jax.random.uniform(key_of[3], (LEVELS,), jnp.float32, math.log(1.5), math.log(4.0))), 1.5, 4.0)
    skeleton = draw_skeleton(jax.random.fold_in(key_of[5], 71), 0)
    return {"embeddings": embeddings, "noise": noise, "targets": targets, "level_scale": level_scale, "skeleton": skeleton}


def kern(left, right):
    left_sq = lax.optimization_barrier(jnp.sum(jnp.square(left.astype(jnp.float32)), axis=1))
    right_sq = lax.optimization_barrier(jnp.sum(jnp.square(right.astype(jnp.float32)), axis=1))
    cross = jnp.dot(left.astype(jnp.float32), right.T.astype(jnp.float32), preferred_element_type=jnp.float32)
    return jnp.exp(-(left_sq[:, None] + right_sq[None, :] - 2.0 * cross) / left.shape[1])

def reference(embeddings, noise, targets, level_scale, skeleton):
    leaves = DEVICES
    blocks = embeddings.reshape(leaves, LEAF, WIDTH)
    noise_blocks = noise.reshape(leaves, LEAF)
    target_blocks = targets.reshape(leaves, LEAF, RHS)
    owner = jnp.arange(leaves, dtype=jnp.int32)
    centers = []
    for level in range(LEVELS):
        group = 2 ** (level + 1)
        picks = skeleton[level, ::group, :]
        centers.append(jnp.take(embeddings, picks, axis=0))
    scales = [jnp.sqrt(level_scale[level] / RANK) for level in range(LEVELS)]

    def leaf_solve(index):
        block = blocks[index]
        gram = kern(block, block) + jnp.diag(noise_blocks[index])
        chol = jnp.linalg.cholesky(gram)
        pieces = []
        for level in range(LEVELS):
            node = index // 2 ** (level + 1)
            pieces.append(kern(block, centers[level][node]) * scales[level])
        pieces.append(target_blocks[index])
        basis = jnp.concatenate(pieces, axis=1)
        solved = jax.scipy.linalg.cho_solve((chol, True), basis)
        return (solved, 2.0 * jnp.sum(jnp.log(jnp.diagonal(chol))))
    solved, leaf_dets = lax.map(leaf_solve, owner)
    total_det = jnp.sum(leaf_dets)
    for level in range(LEVELS):
        group = 2 ** (level + 1)
        nodes = leaves // group
        start = level * RANK
        local = jax.vmap(kern)(blocks, centers[level][owner // group]) * scales[level]
        tail = solved[:, :, start:]
        part = jnp.einsum('bir,bic->brc', local, tail, precision=lax.Precision.HIGHEST)
        sums = part.reshape(nodes, group, RANK, tail.shape[2]).sum(axis=1)
        cap = jnp.eye(RANK, dtype=jnp.float32)[None] + sums[:, :, :RANK]
        capchol = jnp.linalg.cholesky(cap)
        coef = jax.scipy.linalg.cho_solve((capchol, True), sums[:, :, RANK:])
        total_det = total_det + 2.0 * jnp.sum(jnp.log(jnp.diagonal(capchol, axis1=1, axis2=2)))
        shared = coef[owner // group]
        update = jnp.einsum('bir,brc->bic', solved[:, :, start:start + RANK], shared, precision=lax.Precision.HIGHEST)
        solved = jnp.concatenate([solved[:, :, :start + RANK], solved[:, :, start + RANK:] - update], axis=2)
    npoints = leaves * LEAF
    solution = solved[:, :, LEVELS * RANK:].reshape(npoints, RHS)
    fit = lax.optimization_barrier(jnp.sum(targets * solution, axis=0)) / npoints
    logdet = total_det / npoints
    return (solution, fit, logdet)
```

```python
import functools

import jax
import jax.numpy as jnp
from jax import lax
from jax.experimental import pallas as pl
from jax.experimental.pallas import tpu as pltpu
from jax.sharding import PartitionSpec as P

NARROW_WIDE = ("narrow", "wide")
MESH = pl.DeviceIdType.MESH
EXACT = lax.Precision.HIGHEST
CLOSE = lax.Precision.HIGH
LANES = 128
VMEM = pltpu.VMEM


def exact_dot(left, right):
    return jnp.dot(left, right, precision=EXACT, preferred_element_type=jnp.float32)


def unit(k):
    return jnp.where(lax.broadcasted_iota(jnp.int32, (8, LANES), 0) == k, 1.0, 0.0)


def inverse8(cols):
    cols = list(cols)
    logs = jnp.zeros((1, LANES), jnp.float32)
    for k in range(0, 8, 2):
        a, e = cols[k][k : k + 1], cols[k][k + 1 : k + 2]
        b, c = cols[k + 1][k : k + 1], cols[k + 1][k + 1 : k + 2]
        det = a * c - b * e
        inv = 1.0 / det
        logs = logs + jnp.log(det)
        ai, bi, ci, ei = a * inv, b * inv, c * inv, e * inv
        first, second = cols[k] - unit(k), cols[k + 1] - unit(k + 1)
        m0 = first * ci - second * ei
        m1 = second * ai - first * bi
        for j in range(8):
            if j == k:
                cols[j] = unit(k) - m0
            elif j == k + 1:
                cols[j] = unit(k + 1) - m1
            else:
                cols[j] = cols[j] - m0 * cols[j][k : k + 1] - m1 * cols[j][k + 1 : k + 2]
    return cols, logs


def inverse128(load, store, spread_ref):
    lane = lax.broadcasted_iota(jnp.int32, (8, LANES), 1)
    sub = lax.broadcasted_iota(jnp.int32, (8, LANES), 0)
    tiles = LANES // 8
    state = [load(q) for q in range(tiles)]
    total = jnp.zeros((1, LANES), jnp.float32)
    for p in range(tiles):
        cols = [
            [jnp.broadcast_to(state[q][:, 8 * p + j : 8 * p + j + 1], (8, LANES)) for j in range(8)]
            for q in range(tiles)
        ]
        for j in range(8):
            spread_ref[j] = cols[p][j]
        block, logs = inverse8([spread_ref[j] for j in range(8)])
        total = total + logs
        inside = (lane >= 8 * p) & (lane < 8 * p + 8)
        pivot_rows = jnp.where(inside, jnp.where(lane - 8 * p == sub, 1.0, 0.0), state[p])
        scaled = block[0] * pivot_rows[0:1]
        for j in range(1, 8):
            scaled = scaled + block[j] * pivot_rows[j : j + 1]
        rows = [jnp.broadcast_to(scaled[j : j + 1], (8, LANES)) for j in range(8)]
        for q in range(tiles):
            if q == p:
                state[q] = scaled
            else:
                rest = jnp.where(inside, 0.0, state[q])
                for j in range(8):
                    rest = rest - cols[q][j] * rows[j]
                state[q] = rest
    for q in range(tiles):
        store(q, state[q])
    return total


def inverse_kernel(matrix_ref, out_ref, log_ref, spread_ref):
    out_ref[...] = matrix_ref[...]
    log_ref[...] = jnp.zeros_like(log_ref)
    half = out_ref.shape[0] // 2

    def step(j, carry):
        here = pl.ds(pl.multiple_of(j * half, half), half)
        there = pl.ds(pl.multiple_of((1 - j) * half, half), half)

        def rows(q):
            return pl.ds(pl.multiple_of(j * half + 8 * q, 8), 8)

        def store(q, value):
            out_ref[rows(q), here] = value

        log_ref[0:1, :] += inverse128(lambda q: out_ref[rows(q), here], store, spread_ref)
        inv = out_ref[here, here]
        scaled = exact_dot(inv, out_ref[here, there])
        below = out_ref[there, here]
        out_ref[there, there] = out_ref[there, there] - exact_dot(below, scaled)
        out_ref[there, here] = -exact_dot(below, inv)
        out_ref[here, there] = scaled
        return carry

    lax.fori_loop(0, 2, step, 0)


def spd_inverse(matrix):
    order = matrix.shape[0]
    assert order == 2 * LANES
    inverse, logs = pl.pallas_call(
        inverse_kernel,
        out_shape=(
            jax.ShapeDtypeStruct((order, order), jnp.float32),
            jax.ShapeDtypeStruct((8, LANES), jnp.float32),
        ),
        in_specs=[pl.BlockSpec(memory_space=VMEM)],
        out_specs=(pl.BlockSpec(memory_space=VMEM), pl.BlockSpec(memory_space=VMEM)),
        scratch_shapes=[VMEM((8, 8, LANES), jnp.float32)],
        cost_estimate=pl.CostEstimate(flops=60_000_000, bytes_accessed=600_000, transcendentals=512),
        name="spd_inverse",
    )(matrix)
    return inverse, logs[0, 0]


def near_far(level):
    near = min(2**level, 16)
    return near, 2**level // near


def near_peer(near, k):
    narrow, wide = lax.axis_index("narrow"), lax.axis_index("wide")
    here = lax.rem(wide, near)
    peer = lax.rem(here + k, near)
    return here, peer, (narrow, wide - here + peer)


def far_peer(far, k):
    narrow, wide = lax.axis_index("narrow"), lax.axis_index("wide")
    slab, inner = lax.div(wide, 16), lax.rem(wide, 16)
    index = slab if far <= 4 else narrow * 4 + slab
    here = lax.rem(index, far)
    peer = index - here + lax.rem(here + k, far)
    if far <= 4:
        return here, (narrow, peer * 16 + inner)
    return here, (lax.div(peer, 4), lax.rem(peer, 4) * 16 + inner)


def remote(src, dst, send_sem, recv_sem, device):
    return pltpu.make_async_remote_copy(
        src_ref=src, dst_ref=dst, send_sem=send_sem, recv_sem=recv_sem, device_id=device, device_id_type=MESH
    )


def greet(near, far):
    barrier = pltpu.get_barrier_semaphore()
    for k in range(1, near):
        pl.semaphore_signal(barrier, inc=1, device_id=near_peer(near, k)[2], device_id_type=MESH)
    for k in range(1, far):
        pl.semaphore_signal(barrier, inc=1, device_id=far_peer(far, k)[1], device_id_type=MESH)
    pl.semaphore_wait(barrier, near + far - 2)


def node_sum_kernel(near, far, part_ref, out_ref, landed, passed, own, *sems):
    rows = part_ref.shape[0] // near

    def block(index):
        return pl.ds(pl.multiple_of(index * rows, rows), rows)

    scatter_send, scatter_recv, gather_send, gather_recv = sems[:4]
    greet(near, far)
    here = near_peer(near, 0)[0]
    copies = []
    for k in range(1, near):
        _, peer, device = near_peer(near, k)
        copies.append(
            remote(part_ref.at[block(peer)], landed.at[k - 1], scatter_send.at[k - 1], scatter_recv.at[k - 1], device)
        )
        copies[-1].start()
    total = part_ref[block(here)].astype(jnp.float32)
    for k in range(1, near):
        copies[k - 1].wait()
        total = total + landed[k - 1].astype(jnp.float32)
    if far > 1:
        far_send, far_recv = sems[4:]
        own[...] = total.astype(jnp.bfloat16)
        copies = []
        for k in range(1, far):
            copies.append(
                remote(own, passed.at[k - 1], far_send.at[k - 1], far_recv.at[k - 1], far_peer(far, k)[1])
            )
            copies[-1].start()
        total = own[...].astype(jnp.float32)
        for k in range(1, far):
            copies[k - 1].wait()
            total = total + passed[k - 1].astype(jnp.float32)
    out_ref[block(here)] = total.astype(jnp.bfloat16)
    copies = []
    for k in range(1, near):
        device = near_peer(near, k)[2]
        mine = out_ref.at[block(here)]
        copies.append(remote(mine, mine, gather_send.at[k - 1], gather_recv.at[k - 1], device))
        copies[-1].start()
    for copy in copies:
        copy.wait()


def node_sum(part, level):
    near, far = near_far(level)
    order, columns = part.shape
    rows = order // near
    dma = pltpu.SemaphoreType.DMA
    sems = [dma((near - 1,)) for _ in range(4)] + ([dma((far - 1,)) for _ in range(2)] if far > 1 else [])
    return pl.pallas_call(
        functools.partial(node_sum_kernel, near, far),
        out_shape=jax.ShapeDtypeStruct((order, columns), jnp.bfloat16),
        in_specs=[pl.BlockSpec(memory_space=VMEM)],
        out_specs=pl.BlockSpec(memory_space=VMEM),
        scratch_shapes=[
            VMEM((near - 1, rows, columns), jnp.bfloat16),
            VMEM((max(far - 1, 1), rows, columns), jnp.bfloat16),
            VMEM((rows, columns), jnp.bfloat16),
            *sems,
        ],
        compiler_params=pltpu.CompilerParams(collective_id=level, has_side_effects=True),
        name=f"node_sum_{level}",
    )(part)


def whole_sum_kernel(near, far, part_ref, out_ref, landed, passed, own, near_send, near_recv, far_send, far_recv):
    greet(near, far)
    here = near_peer(near, 0)[0]
    landed[here] = part_ref[...]
    copies = []
    for k in range(1, near):
        copies.append(
            remote(part_ref, landed.at[here], near_send.at[k - 1], near_recv.at[k - 1], near_peer(near, k)[2])
        )
        copies[-1].start()
    for copy in copies:
        copy.wait()
    total = landed[0]
    for k in range(1, near):
        total = total + landed[k]
    own[...] = total
    index = far_peer(far, 0)[0]
    passed[index] = total
    copies = []
    for k in range(1, far):
        copies.append(remote(own, passed.at[index], far_send.at[k - 1], far_recv.at[k - 1], far_peer(far, k)[1]))
        copies[-1].start()
    for copy in copies:
        copy.wait()
    total = passed[0]
    for k in range(1, far):
        total = total + passed[k]
    out_ref[...] = total


def whole_sum(part):
    near, far = near_far(7)
    dma = pltpu.SemaphoreType.DMA
    return pl.pallas_call(
        functools.partial(whole_sum_kernel, near, far),
        out_shape=jax.ShapeDtypeStruct(part.shape, jnp.float32),
        in_specs=[pl.BlockSpec(memory_space=VMEM)],
        out_specs=pl.BlockSpec(memory_space=VMEM),
        scratch_shapes=[
            VMEM((near, *part.shape), jnp.float32),
            VMEM((far, *part.shape), jnp.float32),
            VMEM(part.shape, jnp.float32),
            dma((near - 1,)),
            dma((near - 1,)),
            dma((far - 1,)),
            dma((far - 1,)),
        ],
        compiler_params=pltpu.CompilerParams(collective_id=8, has_side_effects=True),
        name="whole_sum",
    )(part)


def partner(value, axis, apart):
    mask = 2**apart
    pairs = [(source, source ^ mask) for source in range(lax.axis_size(axis))]
    return lax.ppermute(value, axis, pairs)


def kern(left, right):
    left_sq = jnp.sum(jnp.square(left.astype(jnp.float32)), axis=1)
    right_sq = jnp.sum(jnp.square(right.astype(jnp.float32)), axis=1)
    cross = jnp.dot(left, right.T, preferred_element_type=jnp.float32)
    return jnp.exp(-(left_sq[:, None] + right_sq[None, :] - 2.0 * cross) / left.shape[1])


def close_dot(left, right):
    return jnp.dot(left, right, precision=CLOSE, preferred_element_type=jnp.float32)


def per_device(embeddings, noise, targets, level_scale, skeleton):
    leaf, width = embeddings.shape
    rank = skeleton.shape[2]
    levels = skeleton.shape[0]
    rhs = targets.shape[1]
    wide_size = lax.axis_size("wide")
    wide_bits = wide_size.bit_length() - 1
    device = lax.axis_index("narrow") * wide_size + lax.axis_index("wide")
    local_index = skeleton[:, 0, :].reshape(-1) - device * leaf
    chosen = (local_index[:, None] == jnp.arange(leaf, dtype=jnp.int32)[None, :]).astype(jnp.bfloat16)
    centers = jnp.dot(chosen, embeddings, preferred_element_type=jnp.float32)
    centers = centers.astype(jnp.bfloat16).reshape(levels, rank, width)
    for bit in range(wide_bits):
        pending = centers[bit:]
        centers = centers.at[bit:].set(pending + partner(pending, "wide", bit))
    topmost = centers[levels - 1 :]
    centers = centers.at[levels - 1 :].set(topmost + partner(topmost, "narrow", 0))
    gram = kern(embeddings, embeddings) + jnp.diag(noise)
    leaf_inverse, det_term = spd_inverse(gram)
    scales = jnp.repeat(jnp.sqrt(level_scale / rank), rank)
    bases = kern(embeddings, centers.reshape(levels * rank, width)) * scales[None, :]
    padded = jnp.pad(targets, ((0, 0), (0, LANES - rhs)))
    solved = exact_dot(leaf_inverse, jnp.concatenate([bases, padded], axis=1))
    for level in range(levels):
        start = level * rank
        base = bases[:, start : start + rank]
        part = close_dot(base.T, solved)
        summed = node_sum(part.astype(jnp.bfloat16), level + 1).astype(jnp.float32)
        cap = jnp.eye(rank, dtype=jnp.float32) + summed[:, :rank]
        cap_inverse, cap_log = spd_inverse(cap)
        coef = close_dot(cap_inverse, summed[:, rank:])
        solved = solved[:, rank:] - close_dot(solved[:, :rank], coef)
        det_term = det_term + cap_log / 2 ** (level + 1)
    answer = solved[:, :rhs]
    fit_term = jnp.sum(targets * answer, axis=0)
    totals = jnp.zeros((8, LANES), jnp.float32).at[0, :rhs].set(fit_term).at[1, 0].set(det_term)
    totals = whole_sum(totals)
    npoints = leaf * lax.axis_size("narrow") * wide_size
    return (answer, totals[0, :rhs] / npoints, totals[1, 0] / npoints)


def solution(mesh):
    return jax.shard_map(
        per_device,
        mesh=mesh,
        in_specs=(
            P(NARROW_WIDE, None),
            P(NARROW_WIDE),
            P(NARROW_WIDE, None),
            P(),
            P(None, NARROW_WIDE, None),
        ),
        out_specs=(P(NARROW_WIDE, None), P(), P()),
        check_vma=False,
    )
```

```python
import functools

import jax
import jax.numpy as jnp
from jax import lax
from jax.experimental import pallas as pl
from jax.experimental.pallas import tpu as pltpu
from jax.sharding import PartitionSpec as P

NARROW_WIDE = ("narrow", "wide")
MESH = pl.DeviceIdType.MESH
EXACT = lax.Precision.HIGHEST
CLOSE = lax.Precision.HIGH
LANES = 128
VMEM = pltpu.VMEM


def exact_dot(left, right):
    return jnp.dot(left, right, precision=EXACT, preferred_element_type=jnp.float32)


def unit(k):
    return jnp.where(lax.broadcasted_iota(jnp.int32, (8, LANES), 0) == k, 1.0, 0.0)


def inverse8(cols):
    cols = list(cols)
    logs = jnp.zeros((1, LANES), jnp.float32)
    for k in range(0, 8, 2):
        a, e = cols[k][k : k + 1], cols[k][k + 1 : k + 2]
        b, c = cols[k + 1][k : k + 1], cols[k + 1][k + 1 : k + 2]
        det = a * c - b * e
        inv = 1.0 / det
        logs = logs + jnp.log(det)
        ai, bi, ci, ei = a * inv, b * inv, c * inv, e * inv
        first, second = cols[k] - unit(k), cols[k + 1] - unit(k + 1)
        m0 = first * ci - second * ei
        m1 = second * ai - first * bi
        for j in range(8):
            if j == k:
                cols[j] = unit(k) - m0
            elif j == k + 1:
                cols[j] = unit(k + 1) - m1
            else:
                cols[j] = cols[j] - m0 * cols[j][k : k + 1] - m1 * cols[j][k + 1 : k + 2]
    return cols, logs


def inverse128(state, spread_ref):
    order = state.shape[0]
    lane = lax.broadcasted_iota(jnp.int32, (order, LANES), 1)
    row = lax.broadcasted_iota(jnp.int32, (order, LANES), 0)
    total = jnp.zeros((1, LANES), jnp.float32)
    for first in range(0, order, 8):
        last = first + 8
        cols = [jnp.broadcast_to(state[:, j : j + 1], (order, LANES)) for j in range(first, last)]
        for j in range(8):
            spread_ref[j] = cols[j][first:last]
        block, logs = inverse8([spread_ref[j] for j in range(8)])
        total = total + logs
        inside = (lane >= first) & (lane < last)
        cleared = jnp.where(inside, jnp.where(lane == row, 1.0, 0.0), state)
        scaled = block[0] * cleared[first : first + 1]
        for j in range(1, 8):
            scaled = scaled + block[j] * cleared[first + j : first + j + 1]
        rest = jnp.where(inside, 0.0, state)
        for j in range(8):
            rest = rest - cols[j] * scaled[j : j + 1]
        pieces = [rest[:first], scaled, rest[last:]]
        state = jnp.concatenate([piece for piece in pieces if piece.shape[0]], axis=0)
    return state, total


def gauss_jordan(matrix_ref, spread_ref, log_ref):
    half = matrix_ref.shape[0] // 2
    log_ref[...] = jnp.zeros_like(log_ref)

    def step(j, carry):
        here = pl.ds(pl.multiple_of(j * half, half), half)
        there = pl.ds(pl.multiple_of((1 - j) * half, half), half)
        inv, logs = inverse128(matrix_ref[here, here], spread_ref)
        log_ref[...] += logs
        scaled = exact_dot(inv, matrix_ref[here, there])
        below = matrix_ref[there, here]
        matrix_ref[there, there] = matrix_ref[there, there] - exact_dot(below, scaled)
        matrix_ref[there, here] = -exact_dot(below, inv)
        matrix_ref[here, there] = scaled
        matrix_ref[here, here] = inv
        return carry

    lax.fori_loop(0, 2, step, 0)


def halves(value):
    high = value.astype(jnp.bfloat16)
    return high, (value - high.astype(jnp.float32)).astype(jnp.bfloat16)


def one_dot(left, right):
    return jnp.dot(left, right, preferred_element_type=jnp.float32)


def three_dot(left, right):
    (left_high, left_low), (right_high, right_low) = left, right
    return one_dot(left_high, right_high) + (one_dot(left_high, right_low) + one_dot(left_low, right_high))


def coef_kernel(level, sums_ref, *refs):
    *basis_refs, target_ref, rest_ref, guess_ref = refs
    order = sums_ref.shape[1]
    basis_columns = sums_ref.shape[2] - order - LANES
    bound = 4.0 * 2**level + 1.0
    row = lax.broadcasted_iota(jnp.int32, (order, order), 0)
    lane = lax.broadcasted_iota(jnp.int32, (order, order), 1)
    eye = jnp.where(row == lane, 1.0, 0.0)
    for node in range(sums_ref.shape[0]):
        cap = eye + sums_ref[node, :, :order].astype(jnp.float32)
        spans = jnp.sum(jnp.abs(cap), axis=0, keepdims=True)
        largest = jnp.minimum(jnp.max(spans), bound)
        scale = 2.0 / (1.0 + jnp.full((1, order), largest, jnp.float32))
        rest = eye - cap * scale
        guess_ref[...] = (eye + rest) * scale
        parts = halves(rest)
        rest_ref[...] = three_dot(parts, parts)
        rounds = jnp.int32(2)
        for k in range(3, level + 5):
            rounds += jnp.where(8.0 * (1.0 + largest) > 2.0**k, 1, 0)

        def step(_, carry):
            rest, guess = rest_ref[...], guess_ref[...]
            parts = halves(rest)
            guess_ref[...] = guess + three_dot(parts, halves(guess))
            rest_ref[...] = three_dot(parts, parts)
            return carry

        lax.fori_loop(0, rounds, step, 0)
        high, low = halves(guess_ref[...])
        right = sums_ref[node, :, order:]
        coef = one_dot(high, right) + one_dot(low, right)
        if basis_refs:
            basis_refs[0][node] = coef[:, :basis_columns].astype(jnp.bfloat16)
        target_ref[node] = coef[:, basis_columns:]


def node_coef(sums, level):
    nodes, order, columns = sums.shape
    basis_columns = columns - order - LANES
    basis_out = [jax.ShapeDtypeStruct((nodes, order, basis_columns), jnp.bfloat16)] if basis_columns else []
    out_shape = [*basis_out, jax.ShapeDtypeStruct((nodes, order, LANES), jnp.float32)]
    *basis, target = pl.pallas_call(
        functools.partial(coef_kernel, level),
        out_shape=out_shape,
        in_specs=[pl.BlockSpec(memory_space=VMEM)],
        out_specs=[pl.BlockSpec(memory_space=VMEM)] * len(out_shape),
        scratch_shapes=[VMEM((order, order), jnp.float32), VMEM((order, order), jnp.float32)],
        cost_estimate=pl.CostEstimate(flops=2_000_000_000, bytes_accessed=2_000_000, transcendentals=0),
        name=f"node_coef_{level}",
    )(sums)
    return basis[0] if basis else None, target


LINE = 4


def near_far(level):
    near = min(2**level, 16)
    return near, 2**level // near


def near_peer(near, k):
    narrow, wide = lax.axis_index("narrow"), lax.axis_index("wide")
    here = lax.rem(wide, near)
    peer = lax.rem(here + k, near)
    return here, peer, (narrow, wide - here + peer)


def far_peer(far, k):
    narrow, wide = lax.axis_index("narrow"), lax.axis_index("wide")
    slab, inner = lax.div(wide, 16), lax.rem(wide, 16)
    index = slab if far <= 4 else narrow * 4 + slab
    here = lax.rem(index, far)
    peer = index - here + lax.rem(here + k, far)
    if far <= 4:
        return here, (narrow, peer * 16 + inner)
    return here, (lax.div(peer, 4), lax.rem(peer, 4) * 16 + inner)


def remote(src, dst, send_sem, recv_sem, device):
    return pltpu.make_async_remote_copy(
        src_ref=src, dst_ref=dst, send_sem=send_sem, recv_sem=recv_sem, device_id=device, device_id_type=MESH
    )


def hail(near, far):
    barrier = pltpu.get_barrier_semaphore()
    for k in range(1, near):
        pl.semaphore_signal(barrier, inc=1, device_id=near_peer(near, k)[2], device_id_type=MESH)
    for k in range(1, far):
        pl.semaphore_signal(barrier, inc=1, device_id=far_peer(far, k)[1], device_id_type=MESH)


def all_here(near, far):
    pl.semaphore_wait(pltpu.get_barrier_semaphore(), near + far - 2)


def column_peer(span, k):
    narrow, wide = lax.axis_index("narrow"), lax.axis_index("wide")
    index = lax.rem(lax.div(wide, LINE), span)
    peer = lax.rem(index + k, span)
    return index, peer, (narrow, wide + (peer - index) * LINE)


def prologue_kernel(
    points_ref, rights_ref, gram_ref, index_ref, points_out, rights_out, pair_out, upper_out, inv_out, log_out,
    inv, spread, rows, pair_landed, landed, passed, own, *sems,
):
    point_sems, right_sems, pair_sems, line_sems, inv_sems, column_sems, far_sems, near_sems = (
        sems[i : i + 2] for i in range(0, 16, 2)
    )
    near, far = near_far(7)
    hail(near, far)
    line = near_peer(LINE, 0)[0]
    column = column_peer(4, 0)[0]
    block = line * 4 + column
    all_here(near, far)
    first = []
    for k in range(1, LINE):
        device = near_peer(LINE, k)[2]
        first.append(
            remote(points_ref, points_out.at[line], point_sems[0].at[k - 1], point_sems[1].at[k - 1], device)
        )
        first[-1].start()
    late = []
    for k in range(1, LINE):
        device = near_peer(LINE, k)[2]
        late.append(
            remote(rights_ref, rights_out.at[line], right_sems[0].at[k - 1], right_sems[1].at[k - 1], device)
        )
        late[-1].start()
    points_out[line] = points_ref[...]
    rights_out[line] = rights_ref[...]
    inv[...] = gram_ref[...]
    gauss_jordan(inv, spread, log_out)
    for k in range(1, LINE):
        device = near_peer(LINE, k)[2]
        late.append(remote(inv, inv_out.at[line], inv_sems[0].at[k - 1], inv_sems[1].at[k - 1], device))
    for copy in first:
        copy.wait()
    index = index_ref[...]
    leaf = points_ref.shape[0]
    total = None
    for leaf_at in range(LINE):
        spot = lax.broadcasted_iota(jnp.int32, (index.shape[0], leaf), 1) + leaf_at * leaf
        term = one_dot(jnp.where(spot == index, 1.0, 0.0).astype(jnp.bfloat16), points_out[leaf_at])
        total = term if total is None else total + term
    rows[...] = total.astype(jnp.bfloat16).reshape(rows.shape)

    pair = remote(rows.at[0], pair_landed, pair_sems[0].at[0], pair_sems[1].at[0], column_peer(2, 1)[2])
    pair.start()
    copies = []
    for k in range(1, 4):
        _, peer, device = column_peer(4, k)
        copies.append(
            remote(
                rows.at[pl.ds(1, 4), peer], landed.at[k - 1], column_sems[0].at[k - 1], column_sems[1].at[k - 1], device
            )
        )
        copies[-1].start()
    for copy in late[LINE - 1 :]:
        copy.start()
    inv_out[line] = inv[...]
    total = rows[pl.ds(1, 4), column].astype(jnp.float32)
    for k in range(1, 4):
        copies[k - 1].wait()
        total = total + landed[k - 1].astype(jnp.float32)
    own[...] = total.astype(jnp.bfloat16)
    copies = []
    for k in range(1, far):
        device = far_peer(far, k)[1]
        copies.append(
            remote(own.at[pl.ds(1, 3)], passed.at[k - 1], far_sems[0].at[k - 1], far_sems[1].at[k - 1], device)
        )
        copies[-1].start()
    pair.wait()
    pair_out[line] = (rows[0].astype(jnp.float32) + pair_landed[...].astype(jnp.float32)).astype(jnp.bfloat16)
    for k in range(1, LINE):
        mine = pair_out.at[line]
        late.append(remote(mine, mine, line_sems[0].at[k - 1], line_sems[1].at[k - 1], near_peer(LINE, k)[2]))
        late[-1].start()
    position = far_peer(far, 0)[0]
    sums = [total[1], total[2], total[3]]
    for k in range(1, far):
        copies[k - 1].wait()
        sender = lax.rem(position + far - k, far)
        core = lax.div(sender, 4) == lax.div(position, 4)
        slab = lax.div(sender, 2) == lax.div(position, 2)
        keep = [jnp.where(slab, 1.0, 0.0), jnp.where(core, 1.0, 0.0), 1.0]
        for i in range(3):
            sums[i] = sums[i] + passed[k - 1, i].astype(jnp.float32) * keep[i]
    upper_out[0, block] = total[0].astype(jnp.bfloat16)
    for i in range(3):
        upper_out[i + 1, block] = sums[i].astype(jnp.bfloat16)
    for k in range(1, near):
        mine = upper_out.at[:, block]
        late.append(remote(mine, mine, near_sems[0].at[k - 1], near_sems[1].at[k - 1], near_peer(near, k)[2]))
        late[-1].start()
    for copy in late:
        copy.wait()


def prologue(points, rights, gram, index):
    leaf, width = points.shape
    order = gram.shape[0]
    near, far = near_far(7)
    few = index.shape[0] // 20
    dma = pltpu.SemaphoreType.DMA
    counts = [LINE - 1, LINE - 1, 1, LINE - 1, LINE - 1, 3, far - 1, near - 1]
    return pl.pallas_call(
        prologue_kernel,
        out_shape=(
            jax.ShapeDtypeStruct((LINE, leaf, width), jnp.bfloat16),
            jax.ShapeDtypeStruct((LINE, *rights.shape), jnp.float32),
            jax.ShapeDtypeStruct((LINE, 4, few, width), jnp.bfloat16),
            jax.ShapeDtypeStruct((4, near, few, width), jnp.bfloat16),
            jax.ShapeDtypeStruct((LINE, order, order), jnp.float32),
            jax.ShapeDtypeStruct((1, LANES), jnp.float32),
        ),
        in_specs=[pl.BlockSpec(memory_space=VMEM)] * 4,
        out_specs=(pl.BlockSpec(memory_space=VMEM),) * 6,
        scratch_shapes=[
            VMEM((order, order), jnp.float32),
            VMEM((8, 8, LANES), jnp.float32),
            VMEM((5, 4, few, width), jnp.bfloat16),
            VMEM((4, few, width), jnp.bfloat16),
            VMEM((3, 4, few, width), jnp.bfloat16),
            VMEM((far - 1, 3, few, width), jnp.bfloat16),
            VMEM((4, few, width), jnp.bfloat16),
            *[dma((count,)) for count in counts for _ in range(2)],
        ],
        compiler_params=pltpu.CompilerParams(collective_id=1, has_side_effects=True),
        name="prologue",
    )(points, rights, gram, index)


def level_kernel(
    near, far, basis_coef_ref, target_coef_ref, solved_ref, answer_ref, base_ref, out_ref, solved_out, answer_out,
    part_ref, base_t_ref, landed, passed, own, *sems,
):
    span = near // LINE
    order = part_ref.shape[0]
    rows = order // near
    hail(near, far)
    line = near_peer(LINE, 0)[0]
    column = column_peer(span, 0)[0]

    def block(column):
        return pl.ds(pl.multiple_of((line * span + column) * rows, rows), rows)

    base_high, base_low = halves(base_ref[...].T)
    base_t_ref[...] = base_high
    front = solved_ref[:, :order]
    coef_high, coef_low = halves(target_coef_ref[...])
    answer = answer_ref[...] - (one_dot(front, coef_high) + one_dot(front, coef_low))
    answer_out[...] = answer
    columns = solved_out.shape[1]
    part_ref[:, columns:] = three_dot((base_high, base_low), halves(answer)).astype(jnp.bfloat16)

    def chunk(c, carry):
        here = pl.ds(pl.multiple_of(c * order, order), order)
        old = solved_ref[:, pl.ds(pl.multiple_of((c + 1) * order, order), order)].astype(jnp.float32)
        new = (old - one_dot(solved_ref[:, :order], basis_coef_ref[:, here])).astype(jnp.bfloat16)
        solved_out[:, here] = new
        part_ref[:, here] = one_dot(base_t_ref[...], new).astype(jnp.bfloat16)
        return carry

    lax.fori_loop(0, columns // order, chunk, 0)

    column_send, column_recv, gather_send, gather_recv = sems[:4]
    all_here(near, far)
    copies = []
    for k in range(1, span):
        _, peer, device = column_peer(span, k)
        copies.append(
            remote(part_ref.at[block(peer)], landed.at[k - 1], column_send.at[k - 1], column_recv.at[k - 1], device)
        )
        copies[-1].start()
    total = part_ref[block(column)].astype(jnp.float32)
    for k in range(1, span):
        copies[k - 1].wait()
        total = total + landed[k - 1].astype(jnp.float32)
    if far > 1:
        far_send, far_recv = sems[4:]
        own[...] = total.astype(jnp.bfloat16)
        copies = []
        for k in range(1, far):
            copies.append(
                remote(own, passed.at[k - 1], far_send.at[k - 1], far_recv.at[k - 1], far_peer(far, k)[1])
            )
            copies[-1].start()
        total = own[...].astype(jnp.float32)
        for k in range(1, far):
            copies[k - 1].wait()
            total = total + passed[k - 1].astype(jnp.float32)
    out_ref[block(column)] = total.astype(jnp.bfloat16)
    copies = []
    for k in range(1, near):
        mine = out_ref.at[block(column)]
        copies.append(remote(mine, mine, gather_send.at[k - 1], gather_recv.at[k - 1], near_peer(near, k)[2]))
        copies[-1].start()
    for copy in copies:
        copy.wait()


def level_step(basis_coef, target_coef, solved, answer, base, level):
    near, far = near_far(level)
    span = near // LINE
    order = base.shape[1]
    points, columns = solved.shape[0], solved.shape[1] - order
    rows = order // near
    counts = [span - 1, span - 1, near - 1, near - 1] + ([far - 1, far - 1] if far > 1 else [])
    return pl.pallas_call(
        functools.partial(level_kernel, near, far),
        out_shape=(
            jax.ShapeDtypeStruct((order, columns + LANES), jnp.bfloat16),
            jax.ShapeDtypeStruct((points, columns), jnp.bfloat16),
            jax.ShapeDtypeStruct(answer.shape, jnp.float32),
        ),
        in_specs=[pl.BlockSpec(memory_space=VMEM)] * 5,
        out_specs=(pl.BlockSpec(memory_space=VMEM),) * 3,
        scratch_shapes=[
            VMEM((order, columns + LANES), jnp.bfloat16),
            VMEM((order, points), jnp.bfloat16),
            VMEM((span - 1, rows, columns + LANES), jnp.bfloat16),
            VMEM((max(far - 1, 1), rows, columns + LANES), jnp.bfloat16),
            VMEM((rows, columns + LANES), jnp.bfloat16),
            *[pltpu.SemaphoreType.DMA((count,)) for count in counts],
        ],
        compiler_params=pltpu.CompilerParams(collective_id=level, has_side_effects=True),
        name=f"level_{level}",
    )(basis_coef, target_coef, solved, answer, base)


def last_kernel(
    near, far, cap_ref, terms_ref, out_ref, inv, spread, logs, part, landed, passed, own,
    near_send, near_recv, far_send, far_recv,
):
    hail(near, far)
    inv[...] = cap_ref[...]
    gauss_jordan(inv, spread, logs)
    first = lax.axis_index("narrow") + lax.axis_index("wide") == 0
    weight = jnp.where(first, 0.0, 1.0)
    row = lax.broadcasted_iota(jnp.int32, part.shape, 0)
    part[...] = terms_ref[...] + jnp.where(row == 1, logs[...] * weight, 0.0)
    all_here(near, far)
    here = near_peer(near, 0)[0]
    copies = []
    for k in range(1, near):
        copies.append(
            remote(part, landed.at[here], near_send.at[k - 1], near_recv.at[k - 1], near_peer(near, k)[2])
        )
        copies[-1].start()
    landed[here] = part[...]
    for copy in copies:
        copy.wait()
    total = landed[0]
    for k in range(1, near):
        total = total + landed[k]
    own[...] = total
    index = far_peer(far, 0)[0]
    copies = []
    for k in range(1, far):
        copies.append(remote(own, passed.at[index], far_send.at[k - 1], far_recv.at[k - 1], far_peer(far, k)[1]))
        copies[-1].start()
    passed[index] = total
    for copy in copies:
        copy.wait()
    total = passed[0]
    for k in range(1, far):
        total = total + passed[k]
    out_ref[...] = total


def last_sum(cap, terms):
    near, far = near_far(7)
    dma = pltpu.SemaphoreType.DMA
    return pl.pallas_call(
        functools.partial(last_kernel, near, far),
        out_shape=jax.ShapeDtypeStruct(terms.shape, jnp.float32),
        in_specs=[pl.BlockSpec(memory_space=VMEM)] * 2,
        out_specs=pl.BlockSpec(memory_space=VMEM),
        scratch_shapes=[
            VMEM(cap.shape, jnp.float32),
            VMEM((8, 8, LANES), jnp.float32),
            VMEM((1, LANES), jnp.float32),
            VMEM(terms.shape, jnp.float32),
            VMEM((near, *terms.shape), jnp.float32),
            VMEM((far, *terms.shape), jnp.float32),
            VMEM(terms.shape, jnp.float32),
            dma((near - 1,)),
            dma((near - 1,)),
            dma((far - 1,)),
            dma((far - 1,)),
        ],
        compiler_params=pltpu.CompilerParams(collective_id=8, has_side_effects=True),
        name="last_sum",
    )(cap, terms)


def kern(left, right):
    left_sq = jnp.sum(jnp.square(left.astype(jnp.float32)), axis=-1)
    right_sq = jnp.sum(jnp.square(right.astype(jnp.float32)), axis=-1)
    cross = jnp.einsum("...iw,...jw->...ij", left, right, preferred_element_type=jnp.float32)
    return jnp.exp(-(left_sq[..., :, None] + right_sq[..., None, :] - 2.0 * cross) / left.shape[-1])


def close(spec, left, right):
    return jnp.einsum(spec, left, right, precision=CLOSE, preferred_element_type=jnp.float32)


def plain(spec, left, right):
    return jnp.einsum(spec, left, right, preferred_element_type=jnp.float32)


def pick(points, index):
    chosen = (index[:, None] == jnp.arange(points.shape[0], dtype=jnp.int32)[None, :]).astype(jnp.bfloat16)
    return jnp.dot(chosen, points, preferred_element_type=jnp.float32).astype(jnp.bfloat16)


def per_device(embeddings, noise, targets, level_scale, skeleton):
    leaf, width = embeddings.shape
    levels, _, rank = skeleton.shape
    rhs = targets.shape[1]
    wide_size = lax.axis_size("wide")
    device = lax.axis_index("narrow") * wide_size + lax.axis_index("wide")
    spot = lax.rem(device, LINE)
    quarter = rank // LINE
    scales = jnp.sqrt(level_scale / rank)

    gram = kern(embeddings, embeddings) + jnp.diag(noise)
    local = skeleton[:, 0, :] - (device - spot) * leaf
    padded = jnp.pad(targets, ((0, 0), (0, LANES - rhs))).at[:, rhs].set(local[0].astype(jnp.float32))
    own_rows = lax.dynamic_slice(local[2:], (0, spot * quarter), (levels - 2, quarter))
    blocks, rights, third_centers, upper_centers, inverses, leaf_log = prologue(
        embeddings, padded, gram, own_rows.reshape(-1, 1)
    )
    points = blocks.reshape(LINE * leaf, width)
    pair_index = rights[::2, :, rhs].astype(jnp.int32)
    low = pick(points, jnp.concatenate([pair_index.reshape(-1), local[1]]))
    shared_centers = jnp.concatenate(
        [low[2 * rank :], third_centers.reshape(rank, width), upper_centers.reshape((levels - 3) * rank, width)]
    )
    first_base = kern(blocks.reshape(2, 2 * leaf, width), low[: 2 * rank].reshape(2, rank, width)) * scales[0]
    bases = kern(points, shared_centers) * jnp.repeat(scales[1:], rank)[None, :]
    stacked = jnp.concatenate([first_base.reshape(LINE * leaf, rank), bases], axis=1)
    solved = jnp.einsum(
        "bij,bjc->bic",
        inverses,
        stacked.reshape(LINE, leaf, levels * rank),
        precision=EXACT,
        preferred_element_type=jnp.float32,
    ).astype(jnp.bfloat16)
    answer = jnp.einsum("bij,bjc->bic", inverses, rights, precision=EXACT, preferred_element_type=jnp.float32)

    solved = solved.reshape(2, 2 * leaf, -1)
    answer = answer.reshape(2, 2 * leaf, LANES)
    part = jnp.concatenate(
        [
            plain("nir,nic->nrc", first_base.astype(jnp.bfloat16), solved).astype(jnp.bfloat16),
            close("nir,nic->nrc", first_base, answer).astype(jnp.bfloat16),
        ],
        axis=2,
    )
    basis_coef, target_coef = node_coef(part, 1)
    front = solved[:, :, :rank]
    answer = answer - close("nir,nrc->nic", front.astype(jnp.float32), target_coef)
    solved = (solved[:, :, rank:].astype(jnp.float32) - plain("nir,nrc->nic", front, basis_coef)).astype(jnp.bfloat16)
    solved = solved.reshape(LINE * leaf, -1)
    answer = answer.reshape(LINE * leaf, LANES)
    caps = [lax.dynamic_index_in_dim(part[:, :, :rank], spot // 2, 0, keepdims=False)]
    base = bases[:, :rank]
    part = jnp.concatenate(
        [
            plain("ir,ic->rc", base.astype(jnp.bfloat16), solved).astype(jnp.bfloat16),
            close("ir,ic->rc", base, answer).astype(jnp.bfloat16),
        ],
        axis=1,
    )
    for level in range(2, levels + 1):
        caps.append(part[:, :rank])
        basis_coef, target_coef = node_coef(part[None], level)
        if level < levels:
            base = bases[:, (level - 1) * rank : level * rank]
            part, solved, answer = level_step(basis_coef[0], target_coef[0], solved, answer, base, level + 1)
    front = lax.dynamic_slice(solved, (spot * leaf, 0), (leaf, rank))
    answer = lax.dynamic_slice(answer, (spot * leaf, 0), (leaf, LANES))
    answer = (answer - close("ir,rc->ic", front.astype(jnp.float32), target_coef[0]))[:, :rhs]

    mine = sum(jnp.where(lax.rem(device, 2**bit) == 0, 1, 0) for bit in range(1, levels))
    cap = lax.dynamic_index_in_dim(jnp.stack(caps), mine, 0, keepdims=False).astype(jnp.float32)
    fit_term = jnp.sum(targets * answer, axis=0)
    terms = jnp.zeros((8, LANES), jnp.float32).at[0, :rhs].set(fit_term).at[1].set(leaf_log[0])
    totals = last_sum(jnp.eye(rank, dtype=jnp.float32) + cap, terms)
    npoints = leaf * lax.axis_size("narrow") * wide_size
    return (answer, totals[0, :rhs] / npoints, totals[1, 0] / npoints)


def solution(mesh):
    return jax.shard_map(
        per_device,
        mesh=mesh,
        in_specs=(
            P(NARROW_WIDE, None),
            P(NARROW_WIDE),
            P(NARROW_WIDE, None),
            P(),
            P(None, NARROW_WIDE, None),
        ),
        out_specs=(P(NARROW_WIDE, None), P(), P()),
        check_vma=False,
    )
```

```python
import functools

import jax
import jax.numpy as jnp
from jax import lax
from jax.experimental import pallas as pl
from jax.experimental.pallas import tpu as pltpu
from jax.sharding import PartitionSpec as P

NARROW_WIDE = ("narrow", "wide")
MESH = pl.DeviceIdType.MESH
EXACT = lax.Precision.HIGHEST
CLOSE = lax.Precision.HIGH
LANES = 128
VMEM = pltpu.VMEM


def exact_dot(left, right):
    return jnp.dot(left, right, precision=EXACT, preferred_element_type=jnp.float32)


def unit(k):
    return jnp.where(lax.broadcasted_iota(jnp.int32, (8, LANES), 0) == k, 1.0, 0.0)


def inverse8(cols):
    cols = list(cols)
    logs = jnp.zeros((1, LANES), jnp.float32)
    for k in range(0, 8, 2):
        a, e = cols[k][k : k + 1], cols[k][k + 1 : k + 2]
        b, c = cols[k + 1][k : k + 1], cols[k + 1][k + 1 : k + 2]
        det = a * c - b * e
        inv = 1.0 / det
        logs = logs + jnp.log(det)
        ai, bi, ci, ei = a * inv, b * inv, c * inv, e * inv
        first, second = cols[k] - unit(k), cols[k + 1] - unit(k + 1)
        m0 = first * ci - second * ei
        m1 = second * ai - first * bi
        for j in range(8):
            if j == k:
                cols[j] = unit(k) - m0
            elif j == k + 1:
                cols[j] = unit(k + 1) - m1
            else:
                cols[j] = cols[j] - m0 * cols[j][k : k + 1] - m1 * cols[j][k + 1 : k + 2]
    return cols, logs


def inverse128(state, spread_ref):
    order = state.shape[0]
    lane = lax.broadcasted_iota(jnp.int32, (order, LANES), 1)
    row = lax.broadcasted_iota(jnp.int32, (order, LANES), 0)
    total = jnp.zeros((1, LANES), jnp.float32)
    for first in range(0, order, 8):
        last = first + 8
        cols = [jnp.broadcast_to(state[:, j : j + 1], (order, LANES)) for j in range(first, last)]
        for j in range(8):
            spread_ref[j] = cols[j][first:last]
        block, logs = inverse8([spread_ref[j] for j in range(8)])
        total = total + logs
        inside = (lane >= first) & (lane < last)
        cleared = jnp.where(inside, jnp.where(lane == row, 1.0, 0.0), state)
        scaled = block[0] * cleared[first : first + 1]
        for j in range(1, 8):
            scaled = scaled + block[j] * cleared[first + j : first + j + 1]
        rest = jnp.where(inside, 0.0, state)
        for j in range(8):
            rest = rest - cols[j] * scaled[j : j + 1]
        pieces = [rest[:first], scaled, rest[last:]]
        state = jnp.concatenate([piece for piece in pieces if piece.shape[0]], axis=0)
    return state, total


def gauss_jordan_half(matrix_ref, spread_ref, log_ref, j):
    half = matrix_ref.shape[0] // 2
    here = pl.ds(pl.multiple_of(j * half, half), half)
    there = pl.ds(pl.multiple_of((1 - j) * half, half), half)
    inv, logs = inverse128(matrix_ref[here, here], spread_ref)
    log_ref[...] += logs
    scaled = exact_dot(inv, matrix_ref[here, there])
    below = matrix_ref[there, here]
    matrix_ref[there, there] = matrix_ref[there, there] - exact_dot(below, scaled)
    matrix_ref[there, here] = -exact_dot(below, inv)
    matrix_ref[here, there] = scaled
    matrix_ref[here, here] = inv


def gauss_jordan(matrix_ref, spread_ref, log_ref, between):
    log_ref[...] = jnp.zeros_like(log_ref)

    def step(j, carry):
        gauss_jordan_half(matrix_ref, spread_ref, log_ref, j)
        if between is not None:
            pl.when(j == 0)(between)
        return carry

    lax.fori_loop(0, 2, step, 0)


def halves(value):
    high = value.astype(jnp.bfloat16)
    return high, (value - high.astype(jnp.float32)).astype(jnp.bfloat16)


def one_dot(left, right):
    return jnp.dot(left, right, preferred_element_type=jnp.float32)


def three_dot(left, right):
    (left_high, left_low), (right_high, right_low) = left, right
    return one_dot(left_high, right_high) + (one_dot(left_high, right_low) + one_dot(left_low, right_high))


def newton_start(level, inner, rest_ref, guess_ref):
    order = inner.shape[0]
    row = lax.broadcasted_iota(jnp.int32, (order, order), 0)
    lane = lax.broadcasted_iota(jnp.int32, (order, order), 1)
    eye = jnp.where(row == lane, 1.0, 0.0)
    cap = eye + inner
    spans = jnp.sum(jnp.abs(cap), axis=0, keepdims=True)
    largest = jnp.minimum(jnp.max(spans, axis=1, keepdims=True), 4.0 * 2**level + 1.0)
    scale = 2.0 / (1.0 + largest)
    rest = eye - cap * scale
    guess_ref[...] = (eye + rest) * scale
    parts = halves(rest)
    rest_ref[...] = three_dot(parts, parts)
    return largest, parts


def newton_round(rest_ref, guess_ref, _, carry):
    guess = guess_ref[...]
    parts = halves(rest_ref[...])
    guess_ref[...] = guess + three_dot(parts, halves(guess))
    rest_ref[...] = three_dot(parts, parts)
    return carry


LINE = 4


def near_far(level):
    near = min(2**level, 16)
    return near, 2**level // near


def near_peer(near, k):
    narrow, wide = lax.axis_index("narrow"), lax.axis_index("wide")
    here = lax.rem(wide, near)
    peer = lax.rem(here + k, near)
    return here, peer, (narrow, wide - here + peer)


def far_peer(far, k):
    narrow, wide = lax.axis_index("narrow"), lax.axis_index("wide")
    slab, inner = lax.div(wide, 16), lax.rem(wide, 16)
    index = slab if far <= 4 else narrow * 4 + slab
    here = lax.rem(index, far)
    peer = index - here + lax.rem(here + k, far)
    if far <= 4:
        return here, (narrow, peer * 16 + inner)
    return here, (lax.div(peer, 4), lax.rem(peer, 4) * 16 + inner)


def remote(src, dst, send_sem, recv_sem, device):
    return pltpu.make_async_remote_copy(
        src_ref=src, dst_ref=dst, send_sem=send_sem, recv_sem=recv_sem, device_id=device, device_id_type=MESH
    )


def hail(near, far):
    barrier = pltpu.get_barrier_semaphore()
    for k in range(1, near):
        pl.semaphore_signal(barrier, inc=1, device_id=near_peer(near, k)[2], device_id_type=MESH)
    for k in range(1, far):
        pl.semaphore_signal(barrier, inc=1, device_id=far_peer(far, k)[1], device_id_type=MESH)


def all_here(near, far):
    pl.semaphore_wait(pltpu.get_barrier_semaphore(), near + far - 2)


def column_peer(span, k):
    narrow, wide = lax.axis_index("narrow"), lax.axis_index("wide")
    index = lax.rem(lax.div(wide, LINE), span)
    peer = lax.rem(index + k, span)
    return index, peer, (narrow, wide + (peer - index) * LINE)


def prologue_kernel(
    points_ref, rights_ref, gram_ref, index_ref, points_out, rights_out, pair_out, upper_out, inv_out, log_out,
    inv, spread, rows, pair_landed, landed, passed, own, *sems,
):
    point_sems, right_sems, pair_sems, line_sems, inv_sems, column_sems, far_sems, near_sems = (
        sems[i : i + 2] for i in range(0, 16, 2)
    )
    near, far = near_far(7)
    hail(near, far)
    line = near_peer(LINE, 0)[0]
    column = column_peer(4, 0)[0]
    block = line * 4 + column
    all_here(near, far)
    first = []
    for k in range(1, LINE):
        device = near_peer(LINE, k)[2]
        first.append(
            remote(points_ref, points_out.at[line], point_sems[0].at[k - 1], point_sems[1].at[k - 1], device)
        )
        first[-1].start()
    late = []
    for k in range(1, LINE):
        device = near_peer(LINE, k)[2]
        late.append(
            remote(rights_ref, rights_out.at[line], right_sems[0].at[k - 1], right_sems[1].at[k - 1], device)
        )
        late[-1].start()
    points_out[line] = points_ref[...]
    rights_out[line] = rights_ref[...]
    inv[...] = gram_ref[...]
    for k in range(1, LINE):
        device = near_peer(LINE, k)[2]
        late.append(remote(inv, inv_out.at[line], inv_sems[0].at[k - 1], inv_sems[1].at[k - 1], device))
    pair = remote(rows.at[0], pair_landed, pair_sems[0].at[0], pair_sems[1].at[0], column_peer(2, 1)[2])
    copies = []
    for k in range(1, 4):
        _, peer, device = column_peer(4, k)
        copies.append(
            remote(
                rows.at[pl.ds(1, 4), peer], landed.at[k - 1], column_sems[0].at[k - 1], column_sems[1].at[k - 1], device
            )
        )

    def choose():
        for copy in first:
            copy.wait()
        index = index_ref[...]
        leaf = points_ref.shape[0]
        total = None
        for leaf_at in range(LINE):
            spot = lax.broadcasted_iota(jnp.int32, (index.shape[0], leaf), 1) + leaf_at * leaf
            term = one_dot(jnp.where(spot == index, 1.0, 0.0).astype(jnp.bfloat16), points_out[leaf_at])
            total = term if total is None else total + term
        rows[...] = total.astype(jnp.bfloat16).reshape(rows.shape)
        pair.start()
        for copy in copies:
            copy.start()

    gauss_jordan(inv, spread, log_out, choose)
    for copy in late[LINE - 1 :]:
        copy.start()
    inv_out[line] = inv[...]
    total = rows[pl.ds(1, 4), column].astype(jnp.float32)
    for k in range(1, 4):
        copies[k - 1].wait()
        total = total + landed[k - 1].astype(jnp.float32)
    own[...] = total.astype(jnp.bfloat16)
    copies = []
    for k in range(1, far):
        device = far_peer(far, k)[1]
        copies.append(
            remote(own.at[pl.ds(1, 3)], passed.at[k - 1], far_sems[0].at[k - 1], far_sems[1].at[k - 1], device)
        )
        copies[-1].start()
    pair.wait()
    pair_out[line] = (rows[0].astype(jnp.float32) + pair_landed[...].astype(jnp.float32)).astype(jnp.bfloat16)
    for k in range(1, LINE):
        mine = pair_out.at[line]
        late.append(remote(mine, mine, line_sems[0].at[k - 1], line_sems[1].at[k - 1], near_peer(LINE, k)[2]))
        late[-1].start()
    position = far_peer(far, 0)[0]
    sums = [total[1], total[2], total[3]]
    for k in range(1, far):
        copies[k - 1].wait()
        sender = lax.rem(position + far - k, far)
        core = lax.div(sender, 4) == lax.div(position, 4)
        slab = lax.div(sender, 2) == lax.div(position, 2)
        keep = [jnp.where(slab, 1.0, 0.0), jnp.where(core, 1.0, 0.0), 1.0]
        for i in range(3):
            sums[i] = sums[i] + passed[k - 1, i].astype(jnp.float32) * keep[i]
    upper_out[0, block] = total[0].astype(jnp.bfloat16)
    for i in range(3):
        upper_out[i + 1, block] = sums[i].astype(jnp.bfloat16)
    for k in range(1, near):
        mine = upper_out.at[:, block]
        late.append(remote(mine, mine, near_sems[0].at[k - 1], near_sems[1].at[k - 1], near_peer(near, k)[2]))
        late[-1].start()
    for copy in late:
        copy.wait()


def prologue(points, rights, gram, index):
    leaf, width = points.shape
    order = gram.shape[0]
    near, far = near_far(7)
    few = index.shape[0] // 20
    dma = pltpu.SemaphoreType.DMA
    counts = [LINE - 1, LINE - 1, 1, LINE - 1, LINE - 1, 3, far - 1, near - 1]
    return pl.pallas_call(
        prologue_kernel,
        out_shape=(
            jax.ShapeDtypeStruct((LINE, leaf, width), jnp.bfloat16),
            jax.ShapeDtypeStruct((LINE, *rights.shape), jnp.float32),
            jax.ShapeDtypeStruct((LINE, 4, few, width), jnp.bfloat16),
            jax.ShapeDtypeStruct((4, near, few, width), jnp.bfloat16),
            jax.ShapeDtypeStruct((LINE, order, order), jnp.float32),
            jax.ShapeDtypeStruct((1, LANES), jnp.float32),
        ),
        in_specs=[pl.BlockSpec(memory_space=VMEM)] * 4,
        out_specs=(pl.BlockSpec(memory_space=VMEM),) * 6,
        scratch_shapes=[
            VMEM((order, order), jnp.float32),
            VMEM((8, 8, LANES), jnp.float32),
            VMEM((5, 4, few, width), jnp.bfloat16),
            VMEM((4, few, width), jnp.bfloat16),
            VMEM((3, 4, few, width), jnp.bfloat16),
            VMEM((far - 1, 3, few, width), jnp.bfloat16),
            VMEM((4, few, width), jnp.bfloat16),
            *[dma((count,)) for count in counts for _ in range(2)],
        ],
        compiler_params=pltpu.CompilerParams(collective_id=1, has_side_effects=True),
        name="prologue",
    )(points, rights, gram, index)


def level_shapes(level, order, width):
    near, far = near_far(level)
    span = near // LINE
    rows = order // near
    left = width - (level - 1) * order
    shapes = [VMEM((order, left), jnp.bfloat16)]
    for size in (order, left - order):
        shapes.append(VMEM((span - 1, rows, size), jnp.bfloat16))
        if far > 1:
            shapes += [VMEM((far - 1, rows, size), jnp.bfloat16), VMEM((rows, size), jnp.bfloat16)]
    counts = [span - 1, span - 1, near - 1, near - 1] + ([far - 1, far - 1] if far > 1 else [])
    return shapes + [pltpu.SemaphoreType.DMA((count,)) for count in counts * 2]


class LevelSum:
    def __init__(self, level, part_ref, refs):
        self.near, self.far = near_far(level)
        self.span = self.near // LINE
        self.part, self.sums = part_ref, refs[0]
        order, left = self.sums.shape
        self.rows = order // self.near
        self.start = (level - 1) * order
        self.pieces = ((0, order), (order, left - order))
        many = 3 if self.far > 1 else 1
        self.buffers = (refs[1 : 1 + many], refs[1 + many : 1 + 2 * many])
        sems = refs[1 + 2 * many :]
        self.sems = (sems[: len(sems) // 2], sems[len(sems) // 2 :])
        self.line = near_peer(LINE, 0)[0]
        self.column = column_peer(self.span, 0)[0]

    def block(self, column):
        return pl.ds(pl.multiple_of((self.line * self.span + column) * self.rows, self.rows), self.rows)

    def from_part(self, i, column):
        first, size = self.pieces[i]
        return self.part.at[self.block(column), pl.ds(self.start + first, size)]

    def scatter(self, i):
        send, recv = self.sems[i][:2]
        copies = []
        for k in range(1, self.span):
            _, peer, device = column_peer(self.span, k)
            landed = self.buffers[i][0].at[k - 1]
            copies.append(remote(self.from_part(i, peer), landed, send.at[k - 1], recv.at[k - 1], device))
            copies[-1].start()
        return copies

    def add_up(self, i, copies):
        total = self.from_part(i, self.column)[...].astype(jnp.float32)
        for k in range(1, self.span):
            copies[k - 1].wait()
            total = total + self.buffers[i][0][k - 1].astype(jnp.float32)
        return total

    def pass_on(self, i, total):
        _, passed, own = self.buffers[i]
        send, recv = self.sems[i][4:6]
        own[...] = total.astype(jnp.bfloat16)
        copies = []
        for k in range(1, self.far):
            device = far_peer(self.far, k)[1]
            copies.append(remote(own, passed.at[k - 1], send.at[k - 1], recv.at[k - 1], device))
            copies[-1].start()
        return copies

    def add_far(self, i, copies):
        _, passed, own = self.buffers[i]
        total = own[...].astype(jnp.float32)
        for k in range(1, self.far):
            copies[k - 1].wait()
            total = total + passed[k - 1].astype(jnp.float32)
        return total

    def gather(self, i, total):
        first, size = self.pieces[i]
        mine = self.sums.at[self.block(self.column), pl.ds(first, size)]
        mine[...] = total.astype(jnp.bfloat16)
        send, recv = self.sems[i][2:4]
        copies = []
        for k in range(1, self.near):
            copies.append(remote(mine, mine, send.at[k - 1], recv.at[k - 1], near_peer(self.near, k)[2]))
            copies[-1].start()
        return copies


def tree_kernel(levels, first_ref, bases_ref, rights_ref, inv_ref, targets_ref, log_ref, answer_out, totals_out, *refs):
    solved, answer, basis_coef, target_coef, part, base_t, rest, guess, cap, spread, logs = refs[:11]
    last = refs[11:19]
    level_refs, at = {}, 19
    order, width = part.shape
    for level in range(3, levels + 1):
        count = len(level_shapes(level, order, width))
        level_refs[level] = refs[at : at + count]
        at += count
    leaf = inv_ref.shape[1]
    tail = levels * order
    near, far = near_far(levels)
    device = lax.axis_index("narrow") * lax.axis_size("wide") + lax.axis_index("wide")
    spot = lax.rem(device, LINE)
    hail(near, far)

    def columns(c):
        return pl.ds(pl.multiple_of(c * order, order), order)

    def leaf_solve(j, carry):
        rows = pl.ds(pl.multiple_of(j * leaf, leaf), leaf)
        inverse = inv_ref[j]
        parts = halves(inverse)
        answer[rows] = exact_dot(inverse, rights_ref[j])
        solved[rows, :order] = three_dot(parts, halves(first_ref[rows])).astype(jnp.bfloat16)

        def chunk(c, carry):
            right = bases_ref[rows, columns(c - 1)]
            solved[rows, columns(c)] = three_dot(halves(inv_ref[j]), halves(right)).astype(jnp.bfloat16)
            return carry

        return lax.fori_loop(1, levels, chunk, carry)

    lax.fori_loop(0, LINE, leaf_solve, 0)
    cap[...] = jnp.zeros_like(cap)

    def choose_cap(inner, mine):
        keep = jnp.where(mine, 1.0, 0.0)
        cap[...] = inner * keep + cap[...] * (1.0 - keep)

    def invert(level, inner):
        newton_start(level, inner, rest, guess)
        lax.fori_loop(0, level + 4, functools.partial(newton_round, rest, guess), 0)

    def products(base, rows, level):
        high, low = halves(base.T)
        base_t[:, : base.shape[0]] = high
        part[:, tail:] = three_dot((high, low), halves(answer[rows])).astype(jnp.bfloat16)

        def chunk(c, carry):
            left = base_t[:, : base.shape[0]]
            part[:, columns(c)] = one_dot(left, solved[rows, columns(c)]).astype(jnp.bfloat16)
            return carry

        lax.fori_loop(level - 1, levels, chunk, 0)

    def solve(level, sums, first, target):
        high, low = halves(guess[...])
        right = sums[:, target:]
        target_coef[...] = one_dot(high, right) + one_dot(low, right)

        def chunk(c, carry):
            right = sums[:, pl.ds(pl.multiple_of(first + (c - level) * order, LANES), order)]
            high, low = halves(guess[...])
            basis_coef[:, columns(c)] = (one_dot(high, right) + one_dot(low, right)).astype(jnp.bfloat16)
            return carry

        lax.fori_loop(level, levels, chunk, 0)

    def take_out_targets(level, rows):
        front = solved[rows, (level - 1) * order : level * order]
        high, low = halves(target_coef[...])
        return answer[rows] - (one_dot(front, high) + one_dot(front, low))

    def take_out(level, rows, c):
        front = solved[rows, (level - 1) * order : level * order]
        old = solved[rows, columns(c)].astype(jnp.float32)
        new = (old - one_dot(front, basis_coef[:, columns(c)])).astype(jnp.bfloat16)
        solved[rows, columns(c)] = new
        return new

    def pair_level(pair, carry):
        rows = pl.ds(pl.multiple_of(pair * 2 * leaf, leaf), 2 * leaf)
        products(first_ref[rows], rows, 1)
        inner = part[:, :order].astype(jnp.float32)
        choose_cap(inner, (pair == lax.div(spot, 2)) & (lax.rem(device, 2) == 1))
        invert(1, inner)
        solve(1, part, order, tail)
        answer[rows] = take_out_targets(1, rows)

        def chunk(c, carry):
            take_out(1, rows, c)
            return carry

        return lax.fori_loop(1, levels, chunk, carry)

    lax.fori_loop(0, 2, pair_level, 0)
    everything = pl.ds(0, LINE * leaf)
    products(bases_ref[:, :order], everything, 2)
    inner = part[:, order : 2 * order].astype(jnp.float32)
    choose_cap(inner, lax.rem(device, 4) == 2)
    invert(2, inner)
    solve(2, part, 2 * order, tail)

    for level in range(3, levels + 1):
        sums = LevelSum(level, part, level_refs[level])
        base_high, base_low = halves(bases_ref[:, (level - 2) * order : (level - 1) * order].T)
        base_t[...] = base_high

        def update(c, carry):
            new = take_out(level - 1, everything, c)
            part[:, columns(c)] = one_dot(base_t[...], new).astype(jnp.bfloat16)
            return carry

        update(level - 1, 0)
        if level == 3:
            all_here(near, far)
        ahead = sums.scatter(0)
        left = take_out_targets(level - 1, everything)
        answer[...] = left
        part[:, tail:] = three_dot((base_high, base_low), halves(left)).astype(jnp.bfloat16)
        lax.fori_loop(level, levels, update, 0)
        behind = sums.scatter(1)
        if sums.far > 1:
            ahead = sums.pass_on(0, sums.add_up(0, ahead))
            behind = sums.pass_on(1, sums.add_up(1, behind))
            ahead = sums.gather(0, sums.add_far(0, ahead))
            behind = sums.gather(1, sums.add_far(1, behind))
        else:
            ahead = sums.gather(0, sums.add_up(0, ahead))
            behind = sums.gather(1, sums.add_up(1, behind))
        for copy in ahead:
            copy.wait()
        inner = sums.sums[:, :order].astype(jnp.float32)
        choose_cap(inner, lax.rem(device, 2**level) == 2 ** (level - 1))
        invert(level, inner)
        for copy in behind:
            copy.wait()
        solve(level, sums.sums, order, tail - (level - 1) * order)

    own_rows = pl.ds(pl.multiple_of(spot * leaf, leaf), leaf)
    own_answer = take_out_targets(levels, own_rows)
    answer_out[...] = own_answer

    landed, passed, terms, own, near_send, near_recv, far_send, far_recv = last
    row = lax.broadcasted_iota(jnp.int32, (order, order), 0)
    lane = lax.broadcasted_iota(jnp.int32, (order, order), 1)
    cap[...] = cap[...] + jnp.where(row == lane, 1.0, 0.0)
    gauss_jordan(cap, spread, logs, None)
    fits = jnp.sum(targets_ref[...] * own_answer, axis=0, keepdims=True)
    line = lax.broadcasted_iota(jnp.int32, terms.shape, 0)
    terms[...] = jnp.where(line == 0, fits, jnp.where(line == 1, logs[...] + log_ref[...], 0.0))
    here = near_peer(near, 0)[0]
    copies = []
    for k in range(1, near):
        device = near_peer(near, k)[2]
        copies.append(remote(terms, landed.at[here], near_send.at[k - 1], near_recv.at[k - 1], device))
        copies[-1].start()
    landed[here] = terms[...]
    for copy in copies:
        copy.wait()
    total = landed[0]
    for k in range(1, near):
        total = total + landed[k]
    own[...] = total
    index = far_peer(far, 0)[0]
    copies = []
    for k in range(1, far):
        copies.append(remote(own, passed.at[index], far_send.at[k - 1], far_recv.at[k - 1], far_peer(far, k)[1]))
        copies[-1].start()
    passed[index] = total
    for copy in copies:
        copy.wait()
    total = passed[0]
    for k in range(1, far):
        total = total + passed[k]
    totals_out[...] = total


def tree(first_base, bases, rights, inverses, targets, leaf_log, levels):
    points, order = first_base.shape
    width = levels * order + LANES
    near, far = near_far(levels)
    dma = pltpu.SemaphoreType.DMA
    terms = (8, LANES)
    scratch = [
        VMEM((points, levels * order), jnp.bfloat16),
        VMEM((points, LANES), jnp.float32),
        VMEM((order, levels * order), jnp.bfloat16),
        VMEM((order, LANES), jnp.float32),
        VMEM((order, width), jnp.bfloat16),
        VMEM((order, points), jnp.bfloat16),
        VMEM((order, order), jnp.float32),
        VMEM((order, order), jnp.float32),
        VMEM((order, order), jnp.float32),
        VMEM((8, 8, LANES), jnp.float32),
        VMEM((1, LANES), jnp.float32),
        VMEM((near, *terms), jnp.float32),
        VMEM((far, *terms), jnp.float32),
        VMEM(terms, jnp.float32),
        VMEM(terms, jnp.float32),
        *[dma((count - 1,)) for count in (near, near, far, far)],
    ]
    for level in range(3, levels + 1):
        scratch += level_shapes(level, order, width)
    return pl.pallas_call(
        functools.partial(tree_kernel, levels),
        out_shape=(jax.ShapeDtypeStruct(targets.shape, jnp.float32), jax.ShapeDtypeStruct(terms, jnp.float32)),
        in_specs=[pl.BlockSpec(memory_space=VMEM)] * 6,
        out_specs=(pl.BlockSpec(memory_space=VMEM),) * 2,
        scratch_shapes=scratch,
        compiler_params=pltpu.CompilerParams(
            collective_id=2, has_side_effects=True, vmem_limit_bytes=56 * 2**20
        ),
        name="tree",
    )(first_base, bases, rights, inverses, targets, leaf_log)


def kern(left, right):
    left_sq = jnp.sum(jnp.square(left.astype(jnp.float32)), axis=-1)
    right_sq = jnp.sum(jnp.square(right.astype(jnp.float32)), axis=-1)
    cross = jnp.einsum("...iw,...jw->...ij", left, right, preferred_element_type=jnp.float32)
    return jnp.exp(-(left_sq[..., :, None] + right_sq[..., None, :] - 2.0 * cross) / left.shape[-1])


def pick(points, index):
    chosen = (index[:, None] == jnp.arange(points.shape[0], dtype=jnp.int32)[None, :]).astype(jnp.bfloat16)
    return jnp.dot(chosen, points, preferred_element_type=jnp.float32).astype(jnp.bfloat16)


def per_device(embeddings, noise, targets, level_scale, skeleton):
    leaf, width = embeddings.shape
    levels, _, rank = skeleton.shape
    rhs = targets.shape[1]
    wide_size = lax.axis_size("wide")
    device = lax.axis_index("narrow") * wide_size + lax.axis_index("wide")
    spot = lax.rem(device, LINE)
    quarter = rank // LINE
    scales = jnp.sqrt(level_scale / rank)

    gram = kern(embeddings, embeddings) + jnp.diag(noise)
    local = skeleton[:, 0, :] - (device - spot) * leaf
    padded = jnp.pad(targets, ((0, 0), (0, LANES - rhs))).at[:, rhs].set(local[0].astype(jnp.float32))
    own_rows = lax.dynamic_slice(local[2:], (0, spot * quarter), (levels - 2, quarter))
    blocks, rights, third_centers, upper_centers, inverses, leaf_log = prologue(
        embeddings, padded, gram, own_rows.reshape(-1, 1)
    )
    points = blocks.reshape(LINE * leaf, width)
    pair_index = rights[::2, :, rhs].astype(jnp.int32)
    low = pick(points, jnp.concatenate([pair_index.reshape(-1), local[1]]))
    shared_centers = jnp.concatenate(
        [low[2 * rank :], third_centers.reshape(rank, width), upper_centers.reshape((levels - 3) * rank, width)]
    )
    first_base = kern(blocks.reshape(2, 2 * leaf, width), low[: 2 * rank].reshape(2, rank, width)) * scales[0]
    bases = kern(points, shared_centers) * jnp.repeat(scales[1:], rank)[None, :]
    answer, totals = tree(
        first_base.reshape(LINE * leaf, rank), bases, rights, inverses, padded, leaf_log, levels
    )
    answer = answer[:, :rhs]
    npoints = leaf * lax.axis_size("narrow") * wide_size
    return (answer, totals[0, :rhs] / npoints, totals[1, 0] / npoints)


def solution(mesh):
    return jax.shard_map(
        per_device,
        mesh=mesh,
        in_specs=(
            P(NARROW_WIDE, None),
            P(NARROW_WIDE),
            P(NARROW_WIDE, None),
            P(),
            P(None, NARROW_WIDE, None),
        ),
        out_specs=(P(NARROW_WIDE, None), P(), P()),
        check_vma=False,
    )
```

```python
import functools

import jax
import jax.numpy as jnp
from jax import lax
from jax.experimental import pallas as pl
from jax.experimental.pallas import tpu as pltpu
from jax.sharding import PartitionSpec as P

NARROW_WIDE = ("narrow", "wide")
MESH = pl.DeviceIdType.MESH
EXACT = lax.Precision.HIGHEST
CLOSE = lax.Precision.HIGH
LANES = 128
VMEM = pltpu.VMEM


def exact_dot(left, right):
    return jnp.dot(left, right, precision=EXACT, preferred_element_type=jnp.float32)


def unit(k):
    return jnp.where(lax.broadcasted_iota(jnp.int32, (8, LANES), 0) == k, 1.0, 0.0)


def inverse8(cols):
    cols = list(cols)
    logs = jnp.zeros((1, LANES), jnp.float32)
    for k in range(0, 8, 2):
        a, e = cols[k][k : k + 1], cols[k][k + 1 : k + 2]
        b, c = cols[k + 1][k : k + 1], cols[k + 1][k + 1 : k + 2]
        det = a * c - b * e
        inv = 1.0 / det
        logs = logs + jnp.log(det)
        ai, bi, ci, ei = a * inv, b * inv, c * inv, e * inv
        first, second = cols[k] - unit(k), cols[k + 1] - unit(k + 1)
        m0 = first * ci - second * ei
        m1 = second * ai - first * bi
        for j in range(8):
            if j == k:
                cols[j] = unit(k) - m0
            elif j == k + 1:
                cols[j] = unit(k + 1) - m1
            else:
                cols[j] = cols[j] - m0 * cols[j][k : k + 1] - m1 * cols[j][k + 1 : k + 2]
    return cols, logs


def inverse128(state, spread_ref, beside):
    order = state.shape[0]
    lane = lax.broadcasted_iota(jnp.int32, (order, LANES), 1)
    row = lax.broadcasted_iota(jnp.int32, (order, LANES), 0)
    total = jnp.zeros((1, LANES), jnp.float32)
    for first in range(0, order, 8):
        last = first + 8
        cols = [jnp.broadcast_to(state[:, j : j + 1], (order, LANES)) for j in range(first, last)]
        for j in range(8):
            spread_ref[j] = cols[j][first:last]
        block, logs = inverse8([spread_ref[j] for j in range(8)])
        total = total + logs
        inside = (lane >= first) & (lane < last)
        cleared = jnp.where(inside, jnp.where(lane == row, 1.0, 0.0), state)
        scaled = block[0] * cleared[first : first + 1]
        for j in range(1, 8):
            scaled = scaled + block[j] * cleared[first + j : first + j + 1]
        rest = jnp.where(inside, 0.0, state)
        for j in range(8):
            rest = rest - cols[j] * scaled[j : j + 1]
        if beside is not None and first % 16 == 8 and first < 96:
            beside()
        pieces = [rest[:first], scaled, rest[last:]]
        state = jnp.concatenate([piece for piece in pieces if piece.shape[0]], axis=0)
    return state, total


def gauss_jordan_half(matrix_ref, spread_ref, log_ref, j, beside):
    half = matrix_ref.shape[0] // 2
    here = pl.ds(pl.multiple_of(j * half, half), half)
    there = pl.ds(pl.multiple_of((1 - j) * half, half), half)
    inv, logs = inverse128(matrix_ref[here, here], spread_ref, beside)
    log_ref[...] += logs
    scaled = exact_dot(inv, matrix_ref[here, there])
    below = matrix_ref[there, here]
    matrix_ref[there, there] = matrix_ref[there, there] - exact_dot(below, scaled)
    matrix_ref[there, here] = -exact_dot(below, inv)
    matrix_ref[here, there] = scaled
    matrix_ref[here, here] = inv


def gauss_jordan(matrix_ref, spread_ref, log_ref, between=None, beside=None):
    log_ref[...] = jnp.zeros_like(log_ref)

    def step(j, carry):
        gauss_jordan_half(matrix_ref, spread_ref, log_ref, j, beside)
        if between is not None:
            pl.when(j == 0)(between)
        return carry

    lax.fori_loop(0, 2, step, 0)


def halves(value):
    high = value.astype(jnp.bfloat16)
    return high, (value - high.astype(jnp.float32)).astype(jnp.bfloat16)


def one_dot(left, right):
    return jnp.dot(left, right, preferred_element_type=jnp.float32)


def three_dot(left, right):
    (left_high, left_low), (right_high, right_low) = left, right
    return one_dot(
        jnp.concatenate([left_high, left_high, left_low], axis=1),
        jnp.concatenate([right_high, right_low, right_high], axis=0),
    )


def newton_start(level, inner, rest_ref, guess_ref):
    order = inner.shape[0]
    row = lax.broadcasted_iota(jnp.int32, (order, order), 0)
    lane = lax.broadcasted_iota(jnp.int32, (order, order), 1)
    eye = jnp.where(row == lane, 1.0, 0.0)
    cap = eye + inner
    spans = jnp.sum(jnp.abs(cap), axis=0, keepdims=True)
    largest = jnp.minimum(jnp.max(spans, axis=1, keepdims=True), 4.0 * 2**level + 1.0)
    scale = 2.0 / (1.0 + largest)
    rest = eye - cap * scale
    guess_ref[...] = (eye + rest) * scale
    parts = halves(rest)
    rest_ref[...] = three_dot(parts, parts)
    return largest, parts


def newton_round(rest_ref, guess_ref, _, carry):
    guess = guess_ref[...]
    parts = halves(rest_ref[...])
    guess_ref[...] = guess + three_dot(parts, halves(guess))
    rest_ref[...] = three_dot(parts, parts)
    return carry


LINE = 4


def near_far(level):
    near = min(2**level, 16)
    return near, 2**level // near


def near_peer(near, k):
    narrow, wide = lax.axis_index("narrow"), lax.axis_index("wide")
    here = lax.rem(wide, near)
    peer = lax.rem(here + k, near)
    return here, peer, (narrow, wide - here + peer)


def far_peer(far, k):
    narrow, wide = lax.axis_index("narrow"), lax.axis_index("wide")
    slab, inner = lax.div(wide, 16), lax.rem(wide, 16)
    index = slab if far <= 4 else narrow * 4 + slab
    here = lax.rem(index, far)
    peer = index - here + lax.rem(here + k, far)
    if far <= 4:
        return here, (narrow, peer * 16 + inner)
    return here, (lax.div(peer, 4), lax.rem(peer, 4) * 16 + inner)


def remote(src, dst, send_sem, recv_sem, device):
    return pltpu.make_async_remote_copy(
        src_ref=src, dst_ref=dst, send_sem=send_sem, recv_sem=recv_sem, device_id=device, device_id_type=MESH
    )


def hail(near, far):
    barrier = pltpu.get_barrier_semaphore()
    for k in range(1, near):
        pl.semaphore_signal(barrier, inc=1, device_id=near_peer(near, k)[2], device_id_type=MESH)
    for k in range(1, far):
        pl.semaphore_signal(barrier, inc=1, device_id=far_peer(far, k)[1], device_id_type=MESH)


def all_here(near, far):
    pl.semaphore_wait(pltpu.get_barrier_semaphore(), near + far - 2)


def column_peer(span, k):
    narrow, wide = lax.axis_index("narrow"), lax.axis_index("wide")
    index = lax.rem(lax.div(wide, LINE), span)
    peer = lax.rem(index + k, span)
    return index, peer, (narrow, wide + (peer - index) * LINE)


def kernel_values(left, right):
    wide_left, wide_right = left.astype(jnp.float32), right.astype(jnp.float32)
    left_sq = jnp.sum(wide_left * wide_left, axis=1, keepdims=True)
    turned = (((1,), (1,)), ((), ()))
    ones = jnp.ones((8, right.shape[1]), jnp.float32)
    right_sq = lax.dot_general(
        ones, wide_right * wide_right, turned, precision=EXACT, preferred_element_type=jnp.float32
    )[0:1]
    cross = lax.dot_general(left, right, turned, preferred_element_type=jnp.float32)
    return jnp.exp(-(left_sq + right_sq - 2.0 * cross) / left.shape[1])


def rows_at(points, index):
    leaf = points.shape[1]
    total = None
    for leaf_at in range(LINE):
        spot = lax.broadcasted_iota(jnp.int32, (index.shape[0], leaf), 1) + leaf_at * leaf
        term = one_dot(jnp.where(spot == index, 1.0, 0.0).astype(jnp.bfloat16), points[leaf_at])
        total = term if total is None else total + term
    return total.astype(jnp.bfloat16)


PROLOGUE_COUNTS = [3, 3, 1, 3, 3, 3, 7, 15]


def prologue(points_ref, rights_ref, noise_ref, index_ref, scales_ref, rights, inv_all, first, bases, log, refs):
    inv, spread, points, pair_all, upper, rows, low, pair_landed, landed, passed, own = refs[:11]
    sems = refs[11:]
    point_sems, right_sems, pair_sems, line_sems, inv_sems, column_sems, far_sems, near_sems = (
        sems[i : i + 2] for i in range(0, 16, 2)
    )
    near, far = near_far(7)
    line = near_peer(LINE, 0)[0]
    column = column_peer(4, 0)[0]
    block = line * 4 + column
    leaf = points_ref.shape[0]
    order = inv.shape[0]

    def to_line(source, target, pair_of_sems):
        send, recv = pair_of_sems
        return [
            remote(source, target, send.at[k - 1], recv.at[k - 1], near_peer(LINE, k)[2]) for k in range(1, LINE)
        ]

    row = lax.broadcasted_iota(jnp.int32, (order, order), 0)
    lane = lax.broadcasted_iota(jnp.int32, (order, order), 1)
    own_points = points_ref[...]
    inv[...] = kernel_values(own_points, own_points) + jnp.where(row == lane, noise_ref[...], 0.0)
    all_here(near, far)
    points_copies = to_line(points_ref, points.at[line], point_sems)
    rights_copies = to_line(rights_ref, rights.at[line], right_sems)
    for copy in points_copies + rights_copies:
        copy.start()
    points[line] = own_points
    rights[line] = rights_ref[...]
    inv_copies = to_line(inv, inv_all.at[line], inv_sems)
    pair = remote(rows.at[0], pair_landed, pair_sems[0].at[0], pair_sems[1].at[0], column_peer(2, 1)[2])
    copies = []
    for k in range(1, 4):
        _, peer, device = column_peer(4, k)
        copies.append(
            remote(
                rows.at[pl.ds(1, 4), peer], landed.at[k - 1], column_sems[0].at[k - 1], column_sems[1].at[k - 1], device
            )
        )

    def choose():
        for copy in points_copies:
            copy.wait()
        rows[...] = rows_at(points, index_ref[order:]).reshape(rows.shape)
        pair.start()
        for copy in copies:
            copy.start()

    gauss_jordan(inv, spread, log, between=choose)
    total = rows[pl.ds(1, 4), column].astype(jnp.float32)
    for k in range(1, 4):
        copies[k - 1].wait()
        total = total + landed[k - 1].astype(jnp.float32)
    own[...] = total.astype(jnp.bfloat16)
    copies = []
    for k in range(1, far):
        device = far_peer(far, k)[1]
        copies.append(
            remote(own.at[pl.ds(1, 3)], passed.at[k - 1], far_sems[0].at[k - 1], far_sems[1].at[k - 1], device)
        )
        copies[-1].start()
    pair.wait()
    pair_all[line] = (rows[0].astype(jnp.float32) + pair_landed[...].astype(jnp.float32)).astype(jnp.bfloat16)
    line_copies = to_line(pair_all.at[line], pair_all.at[line], line_sems)
    for copy in line_copies + inv_copies:
        copy.start()
    inv_all[line] = inv[...]

    def base(level, centers, leaf_at):
        values = kernel_values(points[leaf_at], centers) * scales_ref[level - 1]
        here = pl.ds(pl.multiple_of(leaf_at * leaf, leaf), leaf)
        if level == 1:
            first[here] = values
        else:
            bases[here, (level - 2) * order : (level - 1) * order] = values

    def base_everywhere(level, centers):
        def one(leaf_at, carry):
            base(level, low[...], leaf_at)
            return carry

        low[...] = centers
        lax.fori_loop(0, LINE, one, 0)

    base_everywhere(2, rows_at(points, index_ref[:order]))
    position = far_peer(far, 0)[0]
    sums = [total[1], total[2], total[3]]
    for k in range(1, far):
        copies[k - 1].wait()
        sender = lax.rem(position + far - k, far)
        core = lax.div(sender, 4) == lax.div(position, 4)
        slab = lax.div(sender, 2) == lax.div(position, 2)
        keep = [jnp.where(slab, 1.0, 0.0), jnp.where(core, 1.0, 0.0), 1.0]
        for i in range(3):
            sums[i] = sums[i] + passed[k - 1, i].astype(jnp.float32) * keep[i]
    upper[0, block] = total[0].astype(jnp.bfloat16)
    for i in range(3):
        upper[i + 1, block] = sums[i].astype(jnp.bfloat16)
    near_copies = []
    for k in range(1, near):
        mine = upper.at[:, block]
        near_copies.append(remote(mine, mine, near_sems[0].at[k - 1], near_sems[1].at[k - 1], near_peer(near, k)[2]))
        near_copies[-1].start()
    for copy in rights_copies:
        copy.wait()
    column_of_index = rights_ref.shape[1] // 2

    def pair_base(pair, carry):
        index = rights[2 * pair, :, column_of_index : column_of_index + 1].astype(jnp.int32)
        low[...] = rows_at(points, index)
        base(1, low[...], 2 * pair)
        base(1, low[...], 2 * pair + 1)
        return carry

    lax.fori_loop(0, 2, pair_base, 0)
    for copy in line_copies:
        copy.wait()
    base_everywhere(3, pair_all[...].reshape(order, -1))
    for copy in near_copies:
        copy.wait()
    for level in range(4, 8):
        base_everywhere(level, upper[level - 4].reshape(order, -1))
    for copy in inv_copies:
        copy.wait()


def prologue_shapes(leaf, width, order):
    few = order // 16
    near, far = near_far(7)
    bf16 = jnp.bfloat16
    return [
        VMEM((order, order), jnp.float32),
        VMEM((8, 8, LANES), jnp.float32),
        VMEM((LINE, leaf, width), bf16),
        VMEM((LINE, 4, few, width), bf16),
        VMEM((4, near, few, width), bf16),
        VMEM((5, 4, few, width), bf16),
        VMEM((order, width), bf16),
        VMEM((4, few, width), bf16),
        VMEM((3, 4, few, width), bf16),
        VMEM((far - 1, 3, few, width), bf16),
        VMEM((4, few, width), bf16),
        *[pltpu.SemaphoreType.DMA((count,)) for count in PROLOGUE_COUNTS for _ in range(2)],
    ]


def level_shapes(level, order, left):
    near, far = near_far(level)
    span = near // LINE
    rows = order // near
    shapes = [VMEM((order, left), jnp.bfloat16)]
    for size in (order, left - order):
        shapes.append(VMEM((span - 1, rows, size), jnp.bfloat16))
        if far > 1:
            shapes += [VMEM((far - 1, rows, size), jnp.bfloat16), VMEM((rows, size), jnp.bfloat16)]
    counts = [span - 1, span - 1, near - 1, near - 1] + ([far - 1, far - 1] if far > 1 else [])
    return shapes + [pltpu.SemaphoreType.DMA((count,)) for count in counts * 2]


class LevelSum:
    def __init__(self, level, part_ref, refs):
        self.near, self.far = near_far(level)
        self.span = self.near // LINE
        self.part, self.sums = part_ref, refs[0]
        order, left = self.sums.shape
        self.rows = order // self.near
        self.start = (level - 1) * order
        self.pieces = ((0, order), (order, left - order))
        many = 3 if self.far > 1 else 1
        self.buffers = (refs[1 : 1 + many], refs[1 + many : 1 + 2 * many])
        sems = refs[1 + 2 * many :]
        self.sems = (sems[: len(sems) // 2], sems[len(sems) // 2 :])
        self.line = near_peer(LINE, 0)[0]
        self.column = column_peer(self.span, 0)[0]

    def block(self, column):
        return pl.ds(pl.multiple_of((self.line * self.span + column) * self.rows, self.rows), self.rows)

    def from_part(self, i, column):
        first, size = self.pieces[i]
        return self.part.at[self.block(column), pl.ds(self.start + first, size)]

    def scatter(self, i):
        send, recv = self.sems[i][:2]
        copies = []
        for k in range(1, self.span):
            _, peer, device = column_peer(self.span, k)
            landed = self.buffers[i][0].at[k - 1]
            copies.append(remote(self.from_part(i, peer), landed, send.at[k - 1], recv.at[k - 1], device))
            copies[-1].start()
        return copies

    def add_up(self, i, copies):
        total = self.from_part(i, self.column)[...].astype(jnp.float32)
        for k in range(1, self.span):
            copies[k - 1].wait()
            total = total + self.buffers[i][0][k - 1].astype(jnp.float32)
        return total

    def pass_on(self, i, total):
        _, passed, own = self.buffers[i]
        send, recv = self.sems[i][4:6]
        own[...] = total.astype(jnp.bfloat16)
        copies = []
        for k in range(1, self.far):
            device = far_peer(self.far, k)[1]
            copies.append(remote(own, passed.at[k - 1], send.at[k - 1], recv.at[k - 1], device))
            copies[-1].start()
        return copies

    def add_far(self, i, copies):
        _, passed, own = self.buffers[i]
        total = own[...].astype(jnp.float32)
        for k in range(1, self.far):
            copies[k - 1].wait()
            total = total + passed[k - 1].astype(jnp.float32)
        return total

    def gather(self, i, total):
        first, size = self.pieces[i]
        mine = self.sums.at[self.block(self.column), pl.ds(first, size)]
        mine[...] = total.astype(jnp.bfloat16)
        send, recv = self.sems[i][2:4]
        copies = []
        for k in range(1, self.near):
            copies.append(remote(mine, mine, send.at[k - 1], recv.at[k - 1], near_peer(self.near, k)[2]))
            copies[-1].start()
        return copies


def tree_kernel(levels, points_ref, targets_ref, noise_ref, index_ref, scales_ref, answer_out, totals_out, *refs):
    solved, answer, basis_coef, target_coef, part, base_t, rest, guess, cap, spread, logs = refs[:11]
    last = refs[11:19]
    root_own, root_landed, root_send, root_recv = refs[19:23]
    rights_ref, inv_ref, first_ref, bases_ref, log_ref = refs[23:28]
    begin, at = refs[28:55], 55
    level_refs = {}
    order = part.shape[0]
    width = levels * order + LANES
    for level in range(3, levels):
        count = len(level_shapes(level, order, 2 * order))
        level_refs[level] = refs[at : at + count]
        at += count
    leaf = inv_ref.shape[1]
    tail = levels * order
    near, far = near_far(levels)
    device = lax.axis_index("narrow") * lax.axis_size("wide") + lax.axis_index("wide")
    spot = lax.rem(device, LINE)
    hail(near, far)
    prologue(
        points_ref, targets_ref, noise_ref, index_ref, scales_ref, rights_ref, inv_ref, first_ref, bases_ref, log_ref, begin
    )

    def columns(c):
        return pl.ds(pl.multiple_of(c * order, order), order)

    def leaf_solve(j, carry):
        rows = pl.ds(pl.multiple_of(j * leaf, leaf), leaf)
        inverse = inv_ref[j]
        parts = halves(inverse)
        answer[rows] = exact_dot(inverse, rights_ref[j])
        solved[rows, :order] = three_dot(parts, halves(first_ref[rows])).astype(jnp.bfloat16)

        def chunk(c, carry):
            right = bases_ref[rows, columns(c - 1)]
            solved[rows, columns(c)] = three_dot(halves(inv_ref[j]), halves(right)).astype(jnp.bfloat16)
            return carry

        return lax.fori_loop(1, levels, chunk, carry)

    lax.fori_loop(0, LINE, leaf_solve, 0)
    cap[...] = jnp.zeros_like(cap)

    def choose_cap(inner, mine):
        keep = jnp.where(mine, 1.0, 0.0)
        cap[...] = inner * keep + cap[...] * (1.0 - keep)

    def invert(level, inner):
        newton_start(level, inner, rest, guess)
        lax.fori_loop(0, level + 4, functools.partial(newton_round, rest, guess), 0)

    def products(base, rows, level):
        high, low = halves(base.T)
        base_t[:, : base.shape[0]] = high
        part[:, tail:width] = three_dot((high, low), halves(answer[rows])).astype(jnp.bfloat16)

        def chunk(c, carry):
            left = base_t[:, : base.shape[0]]
            part[:, columns(c)] = one_dot(left, solved[rows, columns(c)]).astype(jnp.bfloat16)
            return carry

        lax.fori_loop(level - 1, levels, chunk, 0)

    def solve(level, sums, first, target):
        high, low = halves(guess[...])
        right = sums[:, target : target + LANES]
        target_coef[...] = one_dot(high, right) + one_dot(low, right)

        def chunk(c, carry):
            right = sums[:, pl.ds(pl.multiple_of(first + (c - level) * order, LANES), order)]
            high, low = halves(guess[...])
            basis_coef[:, columns(c)] = (one_dot(high, right) + one_dot(low, right)).astype(jnp.bfloat16)
            return carry

        lax.fori_loop(level, levels, chunk, 0)

    def take_out_targets(level, rows):
        front = solved[rows, (level - 1) * order : level * order]
        high, low = halves(target_coef[...])
        return answer[rows] - (one_dot(front, high) + one_dot(front, low))

    def take_out(level, rows, c):
        front = solved[rows, (level - 1) * order : level * order]
        old = solved[rows, columns(c)].astype(jnp.float32)
        new = (old - one_dot(front, basis_coef[:, columns(c)])).astype(jnp.bfloat16)
        solved[rows, columns(c)] = new
        return new

    def pair_level(pair, carry):
        rows = pl.ds(pl.multiple_of(pair * 2 * leaf, leaf), 2 * leaf)
        products(first_ref[rows], rows, 1)
        inner = part[:, :order].astype(jnp.float32)
        choose_cap(inner, (pair == lax.div(spot, 2)) & (lax.rem(device, 2) == 1))
        invert(1, inner)
        solve(1, part, order, tail)
        answer[rows] = take_out_targets(1, rows)

        def chunk(c, carry):
            take_out(1, rows, c)
            return carry

        return lax.fori_loop(1, levels, chunk, carry)

    lax.fori_loop(0, 2, pair_level, 0)
    everything = pl.ds(0, LINE * leaf)
    products(bases_ref[:, :order], everything, 2)
    inner = part[:, order : 2 * order].astype(jnp.float32)
    choose_cap(inner, lax.rem(device, 4) == 2)
    invert(2, inner)
    solve(2, part, 2 * order, tail)

    root = levels * order - order
    for level in range(3, levels):
        sums = LevelSum(level, part, level_refs[level])
        base_high, base_low = halves(bases_ref[:, (level - 2) * order : (level - 1) * order].T)
        base_t[...] = base_high

        def update(c, carry):
            new = take_out(level - 1, everything, c)
            part[:, columns(c)] = one_dot(base_t[...], new).astype(jnp.bfloat16)
            return carry

        update(level - 1, 0)
        ahead = sums.scatter(0)
        left = take_out_targets(level - 1, everything)
        answer[...] = left
        part[:, tail:width] = three_dot((base_high, base_low), halves(left)).astype(jnp.bfloat16)
        lax.fori_loop(level, levels, update, 0)
        if level == levels - 1:
            base_high, base_low = halves(bases_ref[:, root - order :].T)
            part[:, width : width + order] = one_dot(base_high, solved[:, root:]).astype(jnp.bfloat16)
            part[:, width + order :] = three_dot((base_high, base_low), halves(left)).astype(jnp.bfloat16)
        behind = sums.scatter(1)
        if sums.far > 1:
            ahead = sums.pass_on(0, sums.add_up(0, ahead))
            behind = sums.pass_on(1, sums.add_up(1, behind))
            ahead = sums.gather(0, sums.add_far(0, ahead))
            behind = sums.gather(1, sums.add_far(1, behind))
        else:
            ahead = sums.gather(0, sums.add_up(0, ahead))
            behind = sums.gather(1, sums.add_up(1, behind))
        for copy in ahead:
            copy.wait()
        inner = sums.sums[:, :order].astype(jnp.float32)
        choose_cap(inner, lax.rem(device, 2**level) == 2 ** (level - 1))
        invert(level, inner)
        for copy in behind:
            copy.wait()
        solve(level, sums.sums, order, tail - (level - 1) * order)

    totals = sums.sums
    high, low = halves(guess[...])
    across = totals[:, order : 2 * order]
    coef = halves(one_dot(high, across) + one_dot(low, across))
    turned = across.astype(jnp.float32).T.astype(jnp.bfloat16)
    root_products = totals[:, 2 * order + LANES :].astype(jnp.float32)
    root_own[:, :order] = root_products[:, :order] - (one_dot(turned, coef[0]) + one_dot(turned, coef[1]))
    coef = halves(target_coef[...])
    root_own[:, order:] = root_products[:, order:] - (one_dot(turned, coef[0]) + one_dot(turned, coef[1]))
    exchange = remote(root_own, root_landed, root_send.at[0], root_recv.at[0], far_peer(far, far // 2)[1])
    exchange.start()
    own_rows = pl.ds(pl.multiple_of(spot * leaf, leaf), leaf)
    answer[own_rows] = take_out_targets(levels - 1, own_rows)
    take_out(levels - 1, own_rows, levels - 1)
    exchange.wait()
    inner = root_own[:, :order] + root_landed[:, :order]
    choose_cap(inner, lax.rem(device, 2**levels) == 2 ** (levels - 1))
    row = lax.broadcasted_iota(jnp.int32, (order, order), 0)
    lane = lax.broadcasted_iota(jnp.int32, (order, order), 1)
    cap[...] = cap[...] + jnp.where(row == lane, 1.0, 0.0)
    newton_start(levels, inner, rest, guess)
    gauss_jordan(cap, spread, logs, beside=functools.partial(newton_round, rest, guess, 0, 0))
    right = root_own[:, order:] + root_landed[:, order:]
    target_coef[...] = three_dot(halves(guess[...]), halves(right))
    own_answer = take_out_targets(levels, own_rows)
    answer_out[...] = own_answer

    landed, passed, terms, own, near_send, near_recv, far_send, far_recv = last
    fits = jnp.sum(targets_ref[...] * own_answer, axis=0, keepdims=True)
    line = lax.broadcasted_iota(jnp.int32, terms.shape, 0)
    terms[...] = jnp.where(line == 0, fits, jnp.where(line == 1, logs[...] + log_ref[...], 0.0))
    here = near_peer(near, 0)[0]
    copies = []
    for k in range(1, near):
        device = near_peer(near, k)[2]
        copies.append(remote(terms, landed.at[here], near_send.at[k - 1], near_recv.at[k - 1], device))
        copies[-1].start()
    landed[here] = terms[...]
    for copy in copies:
        copy.wait()
    total = landed[0]
    for k in range(1, near):
        total = total + landed[k]
    own[...] = total
    index = far_peer(far, 0)[0]
    copies = []
    for k in range(1, far):
        copies.append(remote(own, passed.at[index], far_send.at[k - 1], far_recv.at[k - 1], far_peer(far, k)[1]))
        copies[-1].start()
    passed[index] = total
    for copy in copies:
        copy.wait()
    total = passed[0]
    for k in range(1, far):
        total = total + passed[k]
    totals_out[...] = total


def tree(points, targets, noise, index, scales):
    leaf, feature = points.shape
    levels, order = scales.shape[0], index.shape[0] * 4 // 9
    points_in_line = LINE * leaf
    width = levels * order + LANES
    near, far = near_far(levels)
    dma = pltpu.SemaphoreType.DMA
    terms = (8, LANES)
    scratch = [
        VMEM((points_in_line, levels * order), jnp.bfloat16),
        VMEM((points_in_line, LANES), jnp.float32),
        VMEM((order, levels * order), jnp.bfloat16),
        VMEM((order, LANES), jnp.float32),
        VMEM((order, width + order + LANES), jnp.bfloat16),
        VMEM((order, points_in_line), jnp.bfloat16),
        VMEM((order, order), jnp.float32),
        VMEM((order, order), jnp.float32),
        VMEM((order, order), jnp.float32),
        VMEM((8, 8, LANES), jnp.float32),
        VMEM((1, LANES), jnp.float32),
        VMEM((near, *terms), jnp.float32),
        VMEM((far, *terms), jnp.float32),
        VMEM(terms, jnp.float32),
        VMEM(terms, jnp.float32),
        *[dma((count - 1,)) for count in (near, near, far, far)],
    ]
    scratch += [VMEM((order, order + LANES), jnp.float32)] * 2 + [dma((1,))] * 2
    scratch += [
        VMEM((LINE, leaf, LANES), jnp.float32),
        VMEM((LINE, order, order), jnp.float32),
        VMEM((points_in_line, order), jnp.float32),
        VMEM((points_in_line, (levels - 1) * order), jnp.float32),
        VMEM((1, LANES), jnp.float32),
        *prologue_shapes(leaf, feature, order),
    ]
    for level in range(3, levels):
        extra = order + LANES if level == levels - 1 else 0
        scratch += level_shapes(level, order, width - (level - 1) * order + extra)
    return pl.pallas_call(
        functools.partial(tree_kernel, levels),
        out_shape=(jax.ShapeDtypeStruct((leaf, LANES), jnp.float32), jax.ShapeDtypeStruct(terms, jnp.float32)),
        in_specs=[*[pl.BlockSpec(memory_space=VMEM)] * 4, pl.BlockSpec(memory_space=pltpu.SMEM)],
        out_specs=(pl.BlockSpec(memory_space=VMEM),) * 2,
        scratch_shapes=scratch,
        compiler_params=pltpu.CompilerParams(
            collective_id=2, has_side_effects=True, vmem_limit_bytes=56 * 2**20
        ),
        name="tree",
    )(points, targets, noise, index, scales)


def per_device(embeddings, noise, targets, level_scale, skeleton):
    leaf, _ = embeddings.shape
    levels, _, rank = skeleton.shape
    rhs = targets.shape[1]
    wide_size = lax.axis_size("wide")
    device = lax.axis_index("narrow") * wide_size + lax.axis_index("wide")
    spot = lax.rem(device, LINE)
    quarter = rank // LINE
    scales = jnp.sqrt(level_scale / rank)
    local = skeleton[:, 0, :] - (device - spot) * leaf
    padded = jnp.concatenate(
        [targets, local[0].astype(jnp.float32)[:, None], jnp.zeros((leaf, LANES - rhs - 1), jnp.float32)], axis=1
    )
    own_rows = lax.dynamic_slice(local[2:], (0, spot * quarter), (levels - 2, quarter))
    index = jnp.concatenate([local[1], own_rows.reshape(-1)])[:, None]
    answer, totals = tree(embeddings, padded, noise[None, :], index, scales)
    npoints = leaf * lax.axis_size("narrow") * wide_size
    return (answer[:, :rhs], totals[0, :rhs] / npoints, totals[1, 0] / npoints)


def solution(mesh):
    return jax.shard_map(
        per_device,
        mesh=mesh,
        in_specs=(
            P(NARROW_WIDE, None),
            P(NARROW_WIDE),
            P(NARROW_WIDE, None),
            P(),
            P(None, NARROW_WIDE, None),
        ),
        out_specs=(P(NARROW_WIDE, None), P(), P()),
        check_vma=False,
    )
```

```python
import functools

import jax
import jax.numpy as jnp
from jax import lax
from jax.experimental import pallas as pl
from jax.experimental.pallas import tpu as pltpu
from jax.sharding import PartitionSpec as P

NARROW_WIDE = ("narrow", "wide")
MESH = pl.DeviceIdType.MESH
EXACT = lax.Precision.HIGHEST
CLOSE = lax.Precision.HIGH
LANES = 128
VMEM = pltpu.VMEM


def exact_dot(left, right):
    return jnp.dot(left, right, precision=EXACT, preferred_element_type=jnp.float32)


def unit(k):
    return jnp.where(lax.broadcasted_iota(jnp.int32, (8, LANES), 0) == k, 1.0, 0.0)


def inverse8(cols):
    cols = list(cols)
    logs = jnp.zeros((1, LANES), jnp.float32)
    for k in range(0, 8, 2):
        a, e = cols[k][k : k + 1], cols[k][k + 1 : k + 2]
        b, c = cols[k + 1][k : k + 1], cols[k + 1][k + 1 : k + 2]
        det = a * c - b * e
        inv = 1.0 / det
        logs = logs + jnp.log(det)
        ai, bi, ci, ei = a * inv, b * inv, c * inv, e * inv
        first, second = cols[k] - unit(k), cols[k + 1] - unit(k + 1)
        m0 = first * ci - second * ei
        m1 = second * ai - first * bi
        for j in range(8):
            if j == k:
                cols[j] = unit(k) - m0
            elif j == k + 1:
                cols[j] = unit(k + 1) - m1
            else:
                cols[j] = cols[j] - m0 * cols[j][k : k + 1] - m1 * cols[j][k + 1 : k + 2]
    return cols, logs


def inverse128(state, spread_ref, beside, middle):
    order = state.shape[0]
    lane = lax.broadcasted_iota(jnp.int32, (order, LANES), 1)
    row = lax.broadcasted_iota(jnp.int32, (order, LANES), 0)
    total = jnp.zeros((1, LANES), jnp.float32)
    for first in range(0, order, 8):
        last = first + 8
        cols = [jnp.broadcast_to(state[:, j : j + 1], (order, LANES)) for j in range(first, last)]
        for j in range(8):
            spread_ref[j] = cols[j][first:last]
        block, logs = inverse8([spread_ref[j] for j in range(8)])
        total = total + logs
        inside = (lane >= first) & (lane < last)
        cleared = jnp.where(inside, jnp.where(lane == row, 1.0, 0.0), state)
        scaled = block[0] * cleared[first : first + 1]
        for j in range(1, 8):
            scaled = scaled + block[j] * cleared[first + j : first + j + 1]
        rest = jnp.where(inside, 0.0, state)
        for j in range(8):
            rest = rest - cols[j] * scaled[j : j + 1]
        if beside is not None and first % 16 == 8 and first < 96:
            beside()
        if middle is not None and first == 72:
            middle()
        pieces = [rest[:first], scaled, rest[last:]]
        state = jnp.concatenate([piece for piece in pieces if piece.shape[0]], axis=0)
    return state, total


def gauss_jordan_half(matrix_ref, spread_ref, log_ref, j, beside, middle):
    half = matrix_ref.shape[0] // 2
    here = pl.ds(pl.multiple_of(j * half, half), half)
    there = pl.ds(pl.multiple_of((1 - j) * half, half), half)
    inv, logs = inverse128(matrix_ref[here, here], spread_ref, beside, middle)
    log_ref[...] += logs
    scaled = exact_dot(inv, matrix_ref[here, there])
    below = matrix_ref[there, here]
    matrix_ref[there, there] = matrix_ref[there, there] - exact_dot(below, scaled)
    matrix_ref[there, here] = -exact_dot(below, inv)
    matrix_ref[here, there] = scaled
    matrix_ref[here, here] = inv


def gauss_jordan(matrix_ref, spread_ref, log_ref, between=None, beside=None, later=None):
    log_ref[...] = jnp.zeros_like(log_ref)

    def step(j, carry):
        def middle():
            pl.when(j == 1)(later)

        gauss_jordan_half(matrix_ref, spread_ref, log_ref, j, beside, middle if later is not None else None)
        if between is not None:
            pl.when(j == 0)(between)
        return carry

    lax.fori_loop(0, 2, step, 0)


def halves(value):
    high = value.astype(jnp.bfloat16)
    return high, (value - high.astype(jnp.float32)).astype(jnp.bfloat16)


def one_dot(left, right):
    return jnp.dot(left, right, preferred_element_type=jnp.float32)


def three_dot(left, right):
    (left_high, left_low), (right_high, right_low) = left, right
    return one_dot(
        jnp.concatenate([left_high, left_high, left_low], axis=1),
        jnp.concatenate([right_high, right_low, right_high], axis=0),
    )


def newton_start(level, inner, rest_ref, guess_ref):
    order = inner.shape[0]
    row = lax.broadcasted_iota(jnp.int32, (order, order), 0)
    lane = lax.broadcasted_iota(jnp.int32, (order, order), 1)
    eye = jnp.where(row == lane, 1.0, 0.0)
    cap = eye + inner
    spans = jnp.sum(jnp.abs(cap), axis=0, keepdims=True)
    largest = jnp.minimum(jnp.max(spans, axis=1, keepdims=True), 4.0 * 2**level + 1.0)
    scale = 2.0 / (1.0 + largest)
    rest = eye - cap * scale
    guess_ref[...] = (eye + rest) * scale
    parts = halves(rest)
    rest_ref[...] = three_dot(parts, parts)
    return largest, parts


def newton_round(rest_ref, guess_ref, _, carry):
    guess = guess_ref[...]
    parts = halves(rest_ref[...])
    guess_ref[...] = guess + three_dot(parts, halves(guess))
    rest_ref[...] = three_dot(parts, parts)
    return carry


LINE = 4


def near_far(level):
    near = min(2**level, 16)
    return near, 2**level // near


def near_peer(near, k):
    narrow, wide = lax.axis_index("narrow"), lax.axis_index("wide")
    here = lax.rem(wide, near)
    peer = lax.rem(here + k, near)
    return here, peer, (narrow, wide - here + peer)


def far_peer(far, k):
    narrow, wide = lax.axis_index("narrow"), lax.axis_index("wide")
    slab, inner = lax.div(wide, 16), lax.rem(wide, 16)
    index = slab if far <= 4 else narrow * 4 + slab
    here = lax.rem(index, far)
    peer = index - here + lax.rem(here + k, far)
    if far <= 4:
        return here, (narrow, peer * 16 + inner)
    return here, (lax.div(peer, 4), lax.rem(peer, 4) * 16 + inner)


def remote(src, dst, send_sem, recv_sem, device):
    return pltpu.make_async_remote_copy(
        src_ref=src, dst_ref=dst, send_sem=send_sem, recv_sem=recv_sem, device_id=device, device_id_type=MESH
    )


def hail(near, far):
    barrier = pltpu.get_barrier_semaphore()
    for k in range(1, near):
        pl.semaphore_signal(barrier, inc=1, device_id=near_peer(near, k)[2], device_id_type=MESH)
    for k in range(1, far):
        pl.semaphore_signal(barrier, inc=1, device_id=far_peer(far, k)[1], device_id_type=MESH)


def all_here(near, far):
    pl.semaphore_wait(pltpu.get_barrier_semaphore(), near + far - 2)


def column_peer(span, k):
    narrow, wide = lax.axis_index("narrow"), lax.axis_index("wide")
    index = lax.rem(lax.div(wide, LINE), span)
    peer = lax.rem(index + k, span)
    return index, peer, (narrow, wide + (peer - index) * LINE)


def kernel_values(left, right):
    wide_left, wide_right = left.astype(jnp.float32), right.astype(jnp.float32)
    left_sq = jnp.sum(wide_left * wide_left, axis=1, keepdims=True)
    turned = (((1,), (1,)), ((), ()))
    ones = jnp.ones((8, right.shape[1]), jnp.float32)
    right_sq = lax.dot_general(
        ones, wide_right * wide_right, turned, precision=EXACT, preferred_element_type=jnp.float32
    )[0:1]
    cross = lax.dot_general(left, right, turned, preferred_element_type=jnp.float32)
    return jnp.exp(-(left_sq + right_sq - 2.0 * cross) / left.shape[1])


def rows_at(points, index):
    leaf = points.shape[1]
    total = None
    for leaf_at in range(LINE):
        spot = lax.broadcasted_iota(jnp.int32, (index.shape[0], leaf), 1) + leaf_at * leaf
        term = one_dot(jnp.where(spot == index, 1.0, 0.0).astype(jnp.bfloat16), points[leaf_at])
        total = term if total is None else total + term
    return total.astype(jnp.bfloat16)


PROLOGUE_COUNTS = [3, 3, 1, 3, 3, 3, 7, 15]


def prologue(points_ref, rights_ref, noise_ref, index_ref, scales_ref, rights, inv_all, first, bases, log, refs):
    inv, spread, points, pair_all, upper, rows, low, pair_landed, landed, passed, own = refs[:11]
    sems = refs[11:]
    point_sems, right_sems, pair_sems, line_sems, inv_sems, column_sems, far_sems, near_sems = (
        sems[i : i + 2] for i in range(0, 16, 2)
    )
    near, far = near_far(7)
    line = near_peer(LINE, 0)[0]
    column = column_peer(4, 0)[0]
    block = line * 4 + column
    leaf = points_ref.shape[0]
    order = inv.shape[0]

    def to_line(source, target, pair_of_sems):
        send, recv = pair_of_sems
        return [
            remote(source, target, send.at[k - 1], recv.at[k - 1], near_peer(LINE, k)[2]) for k in range(1, LINE)
        ]

    row = lax.broadcasted_iota(jnp.int32, (order, order), 0)
    lane = lax.broadcasted_iota(jnp.int32, (order, order), 1)
    own_points = points_ref[...]
    inv[...] = kernel_values(own_points, own_points) + jnp.where(row == lane, noise_ref[...], 0.0)
    all_here(near, far)
    points_copies = to_line(points_ref, points.at[line], point_sems)
    rights_copies = to_line(rights_ref, rights.at[line], right_sems)
    for copy in points_copies + rights_copies:
        copy.start()
    points[line] = own_points
    rights[line] = rights_ref[...]
    inv_copies = to_line(inv, inv_all.at[line], inv_sems)
    pair = remote(rows.at[0], pair_landed, pair_sems[0].at[0], pair_sems[1].at[0], column_peer(2, 1)[2])
    copies = []
    for k in range(1, 4):
        _, peer, device = column_peer(4, k)
        copies.append(
            remote(
                rows.at[pl.ds(1, 4), peer], landed.at[k - 1], column_sems[0].at[k - 1], column_sems[1].at[k - 1], device
            )
        )

    def choose():
        for copy in points_copies:
            copy.wait()
        rows[...] = rows_at(points, index_ref[order:]).reshape(rows.shape)
        pair.start()
        for copy in copies:
            copy.start()

    far_copies = []
    for k in range(1, far):
        device = far_peer(far, k)[1]
        far_copies.append(
            remote(own.at[pl.ds(1, 3)], passed.at[k - 1], far_sems[0].at[k - 1], far_sems[1].at[k - 1], device)
        )

    def hand_on():
        total = rows[pl.ds(1, 4), column].astype(jnp.float32)
        for k in range(1, 4):
            copies[k - 1].wait()
            total = total + landed[k - 1].astype(jnp.float32)
        own[...] = total.astype(jnp.bfloat16)
        for copy in far_copies:
            copy.start()

    gauss_jordan(inv, spread, log, between=choose, later=hand_on)
    pair.wait()
    pair_all[line] = (rows[0].astype(jnp.float32) + pair_landed[...].astype(jnp.float32)).astype(jnp.bfloat16)
    line_copies = to_line(pair_all.at[line], pair_all.at[line], line_sems)
    for copy in line_copies + inv_copies:
        copy.start()
    inv_all[line] = inv[...]

    def base(level, centers, leaf_at):
        values = kernel_values(points[leaf_at], centers) * scales_ref[level - 1]
        here = pl.ds(pl.multiple_of(leaf_at * leaf, leaf), leaf)
        if level == 1:
            first[here] = values
        else:
            bases[here, (level - 2) * order : (level - 1) * order] = values

    def base_everywhere(level, centers):
        def one(leaf_at, carry):
            base(level, low[...], leaf_at)
            return carry

        low[...] = centers
        lax.fori_loop(0, LINE, one, 0)

    base_everywhere(2, rows_at(points, index_ref[:order]))
    position = far_peer(far, 0)[0]
    sums = [own[1].astype(jnp.float32), own[2].astype(jnp.float32), own[3].astype(jnp.float32)]
    for k in range(1, far):
        far_copies[k - 1].wait()
        sender = lax.rem(position + far - k, far)
        core = lax.div(sender, 4) == lax.div(position, 4)
        slab = lax.div(sender, 2) == lax.div(position, 2)
        keep = [jnp.where(slab, 1.0, 0.0), jnp.where(core, 1.0, 0.0), 1.0]
        for i in range(3):
            sums[i] = sums[i] + passed[k - 1, i].astype(jnp.float32) * keep[i]
    upper[0, block] = own[0]
    for i in range(3):
        upper[i + 1, block] = sums[i].astype(jnp.bfloat16)
    near_copies = []
    for k in range(1, near):
        mine = upper.at[:, block]
        near_copies.append(remote(mine, mine, near_sems[0].at[k - 1], near_sems[1].at[k - 1], near_peer(near, k)[2]))
        near_copies[-1].start()
    for copy in rights_copies:
        copy.wait()
    column_of_index = rights_ref.shape[1] // 2

    def pair_base(pair, carry):
        index = rights[2 * pair, :, column_of_index : column_of_index + 1].astype(jnp.int32)
        low[...] = rows_at(points, index)
        base(1, low[...], 2 * pair)
        base(1, low[...], 2 * pair + 1)
        return carry

    lax.fori_loop(0, 2, pair_base, 0)
    for copy in line_copies:
        copy.wait()
    base_everywhere(3, pair_all[...].reshape(order, -1))
    for copy in near_copies:
        copy.wait()
    for level in range(4, 8):
        base_everywhere(level, upper[level - 4].reshape(order, -1))
    for copy in inv_copies:
        copy.wait()


def prologue_shapes(leaf, width, order):
    few = order // 16
    near, far = near_far(7)
    bf16 = jnp.bfloat16
    return [
        VMEM((order, order), jnp.float32),
        VMEM((8, 8, LANES), jnp.float32),
        VMEM((LINE, leaf, width), bf16),
        VMEM((LINE, 4, few, width), bf16),
        VMEM((4, near, few, width), bf16),
        VMEM((5, 4, few, width), bf16),
        VMEM((order, width), bf16),
        VMEM((4, few, width), bf16),
        VMEM((3, 4, few, width), bf16),
        VMEM((far - 1, 3, few, width), bf16),
        VMEM((4, few, width), bf16),
        *[pltpu.SemaphoreType.DMA((count,)) for count in PROLOGUE_COUNTS for _ in range(2)],
    ]


def level_shapes(level, order, left):
    near, far = near_far(level)
    span = near // LINE
    rows = order // near
    shapes = [VMEM((order, left), jnp.bfloat16)]
    for size in (order, left - order):
        shapes.append(VMEM((span - 1, rows, size), jnp.bfloat16))
        if far > 1:
            shapes += [VMEM((far - 1, rows, size), jnp.bfloat16), VMEM((rows, size), jnp.bfloat16)]
    counts = [span - 1, span - 1, near - 1, near - 1] + ([far - 1, far - 1] if far > 1 else [])
    return shapes + [pltpu.SemaphoreType.DMA((count,)) for count in counts * 2]


class LevelSum:
    def __init__(self, level, part_ref, refs):
        self.near, self.far = near_far(level)
        self.span = self.near // LINE
        self.part, self.sums = part_ref, refs[0]
        order, left = self.sums.shape
        self.rows = order // self.near
        self.start = (level - 1) * order
        self.pieces = ((0, order), (order, left - order))
        many = 3 if self.far > 1 else 1
        self.buffers = (refs[1 : 1 + many], refs[1 + many : 1 + 2 * many])
        sems = refs[1 + 2 * many :]
        self.sems = (sems[: len(sems) // 2], sems[len(sems) // 2 :])
        self.line = near_peer(LINE, 0)[0]
        self.column = column_peer(self.span, 0)[0]

    def block(self, column):
        return pl.ds(pl.multiple_of((self.line * self.span + column) * self.rows, self.rows), self.rows)

    def from_part(self, i, column):
        first, size = self.pieces[i]
        return self.part.at[self.block(column), pl.ds(self.start + first, size)]

    def scatter(self, i):
        send, recv = self.sems[i][:2]
        copies = []
        for k in range(1, self.span):
            _, peer, device = column_peer(self.span, k)
            landed = self.buffers[i][0].at[k - 1]
            copies.append(remote(self.from_part(i, peer), landed, send.at[k - 1], recv.at[k - 1], device))
            copies[-1].start()
        return copies

    def add_up(self, i, copies):
        total = self.from_part(i, self.column)[...].astype(jnp.float32)
        for k in range(1, self.span):
            copies[k - 1].wait()
            total = total + self.buffers[i][0][k - 1].astype(jnp.float32)
        return total

    def pass_on(self, i, total):
        _, passed, own = self.buffers[i]
        send, recv = self.sems[i][4:6]
        own[...] = total.astype(jnp.bfloat16)
        copies = []
        for k in range(1, self.far):
            device = far_peer(self.far, k)[1]
            copies.append(remote(own, passed.at[k - 1], send.at[k - 1], recv.at[k - 1], device))
            copies[-1].start()
        return copies

    def add_far(self, i, copies):
        _, passed, own = self.buffers[i]
        total = own[...].astype(jnp.float32)
        for k in range(1, self.far):
            copies[k - 1].wait()
            total = total + passed[k - 1].astype(jnp.float32)
        return total

    def gather(self, i, total):
        first, size = self.pieces[i]
        mine = self.sums.at[self.block(self.column), pl.ds(first, size)]
        mine[...] = total.astype(jnp.bfloat16)
        send, recv = self.sems[i][2:4]
        copies = []
        for k in range(1, self.near):
            copies.append(remote(mine, mine, send.at[k - 1], recv.at[k - 1], near_peer(self.near, k)[2]))
            copies[-1].start()
        return copies


def tree_kernel(levels, points_ref, targets_ref, noise_ref, index_ref, scales_ref, answer_out, fit_out, logdet_out, *refs):
    solved, answer, basis_coef, target_coef, part, base_t, rest, guess, cap, spread, logs = refs[:11]
    base_t_low, refs = refs[11], refs[:11] + refs[12:]
    last = refs[11:19]
    root_own, root_landed, root_send, root_recv = refs[19:23]
    rights_ref, inv_ref, first_ref, bases_ref, log_ref = refs[23:28]
    begin, at = refs[28:55], 55
    level_refs = {}
    order = part.shape[0]
    width = levels * order + LANES
    for level in range(3, levels):
        count = len(level_shapes(level, order, 2 * order))
        level_refs[level] = refs[at : at + count]
        at += count
    leaf = inv_ref.shape[1]
    tail = levels * order
    near, far = near_far(levels)
    device = lax.axis_index("narrow") * lax.axis_size("wide") + lax.axis_index("wide")
    spot = lax.rem(device, LINE)
    hail(near, far)
    prologue(
        points_ref, targets_ref, noise_ref, index_ref, scales_ref, rights_ref, inv_ref, first_ref, bases_ref, log_ref, begin
    )

    def columns(c):
        return pl.ds(pl.multiple_of(c * order, order), order)

    def leaf_solve(j, carry):
        rows = pl.ds(pl.multiple_of(j * leaf, leaf), leaf)
        inverse = inv_ref[j]
        parts = halves(inverse)
        answer[rows] = exact_dot(inverse, rights_ref[j])
        solved[rows, :order] = three_dot(parts, halves(first_ref[rows])).astype(jnp.bfloat16)

        def chunk(c, carry):
            right = bases_ref[rows, columns(c - 1)]
            solved[rows, columns(c)] = three_dot(halves(inv_ref[j]), halves(right)).astype(jnp.bfloat16)
            return carry

        return lax.fori_loop(1, levels, chunk, carry)

    lax.fori_loop(0, LINE, leaf_solve, 0)
    cap[...] = jnp.zeros_like(cap)

    def choose_cap(inner, mine):
        keep = jnp.where(mine, 1.0, 0.0)
        cap[...] = inner * keep + cap[...] * (1.0 - keep)

    def invert(level, inner):
        newton_start(level, inner, rest, guess)
        lax.fori_loop(0, level + 4, functools.partial(newton_round, rest, guess), 0)

    def products(base, rows, level):
        high, low = halves(base.T)
        base_t[:, : base.shape[0]] = high
        part[:, tail:width] = three_dot((high, low), halves(answer[rows])).astype(jnp.bfloat16)

        def chunk(c, carry):
            left = base_t[:, : base.shape[0]]
            part[:, columns(c)] = one_dot(left, solved[rows, columns(c)]).astype(jnp.bfloat16)
            return carry

        lax.fori_loop(level - 1, levels, chunk, 0)

    def solve_chunk(level, sums, first, c):
        right = sums[:, pl.ds(pl.multiple_of(first + (c - level) * order, LANES), order)]
        high, low = halves(guess[...])
        basis_coef[:, columns(c)] = (one_dot(high, right) + one_dot(low, right)).astype(jnp.bfloat16)

    def solve_rest(level, sums, first, target):
        high, low = halves(guess[...])
        right = sums[:, target : target + LANES]
        target_coef[...] = one_dot(high, right) + one_dot(low, right)

        def chunk(c, carry):
            solve_chunk(level, sums, first, c)
            return carry

        lax.fori_loop(level + 1, levels, chunk, 0)

    def take_out_targets(level, rows):
        front = solved[rows, (level - 1) * order : level * order]
        high, low = halves(target_coef[...])
        return answer[rows] - (one_dot(front, high) + one_dot(front, low))

    def take_out(level, rows, c):
        front = solved[rows, (level - 1) * order : level * order]
        old = solved[rows, columns(c)].astype(jnp.float32)
        new = (old - one_dot(front, basis_coef[:, columns(c)])).astype(jnp.bfloat16)
        solved[rows, columns(c)] = new
        return new

    def pair_level(pair, carry):
        rows = pl.ds(pl.multiple_of(pair * 2 * leaf, leaf), 2 * leaf)
        products(first_ref[rows], rows, 1)
        inner = part[:, :order].astype(jnp.float32)
        choose_cap(inner, (pair == lax.div(spot, 2)) & (lax.rem(device, 2) == 1))
        invert(1, inner)
        solve_chunk(1, part, order, 1)
        solve_rest(1, part, order, tail)
        answer[rows] = take_out_targets(1, rows)

        def chunk(c, carry):
            take_out(1, rows, c)
            return carry

        return lax.fori_loop(1, levels, chunk, carry)

    lax.fori_loop(0, 2, pair_level, 0)
    everything = pl.ds(0, LINE * leaf)
    products(bases_ref[:, :order], everything, 2)
    inner = part[:, order : 2 * order].astype(jnp.float32)
    choose_cap(inner, lax.rem(device, 4) == 2)
    invert(2, inner)
    solve_chunk(2, part, 2 * order, 2)
    rest_of = (2, part, 2 * order, tail)

    root = levels * order - order

    def turn_base(level):
        base_t[...], base_t_low[...] = halves(bases_ref[:, (level - 2) * order : (level - 1) * order].T)

    turn_base(3)
    for level in range(3, levels):
        sums = LevelSum(level, part, level_refs[level])

        def update(c, carry):
            new = take_out(level - 1, everything, c)
            part[:, columns(c)] = one_dot(base_t[...], new).astype(jnp.bfloat16)
            return carry

        update(level - 1, 0)
        ahead = sums.scatter(0)
        solve_rest(*rest_of)
        left = take_out_targets(level - 1, everything)
        answer[...] = left
        part[:, tail:width] = three_dot((base_t[...], base_t_low[...]), halves(left)).astype(jnp.bfloat16)
        lax.fori_loop(level, levels, update, 0)
        if level == levels - 1:
            base_high, base_low = halves(bases_ref[:, root - order :].T)
            part[:, width : width + order] = one_dot(base_high, solved[:, root:]).astype(jnp.bfloat16)
            part[:, width + order :] = three_dot((base_high, base_low), halves(left)).astype(jnp.bfloat16)
        behind = sums.scatter(1)
        if sums.far > 1:
            ahead = sums.pass_on(0, sums.add_up(0, ahead))
            behind = sums.pass_on(1, sums.add_up(1, behind))
            ahead = sums.gather(0, sums.add_far(0, ahead))
            behind = sums.gather(1, sums.add_far(1, behind))
        else:
            ahead = sums.gather(0, sums.add_up(0, ahead))
            behind = sums.gather(1, sums.add_up(1, behind))
        if level < levels - 1:
            turn_base(level + 1)
        for copy in ahead:
            copy.wait()
        inner = sums.sums[:, :order].astype(jnp.float32)
        choose_cap(inner, lax.rem(device, 2**level) == 2 ** (level - 1))
        invert(level, inner)
        for copy in behind:
            copy.wait()
        rest_of = (level, sums.sums, order, tail - (level - 1) * order)
        if level < levels - 1:
            solve_chunk(level, sums.sums, order, level)

    totals = sums.sums
    solve_chunk(levels - 1, totals, order, levels - 1)
    solve_rest(*rest_of)
    high, low = halves(guess[...])
    across = totals[:, order : 2 * order]
    coef = halves(one_dot(high, across) + one_dot(low, across))
    turned = across.astype(jnp.float32).T.astype(jnp.bfloat16)
    root_products = totals[:, 2 * order + LANES :].astype(jnp.float32)
    root_own[:, :order] = root_products[:, :order] - (one_dot(turned, coef[0]) + one_dot(turned, coef[1]))
    coef = halves(target_coef[...])
    root_own[:, order:] = root_products[:, order:] - (one_dot(turned, coef[0]) + one_dot(turned, coef[1]))
    exchange = remote(root_own, root_landed, root_send.at[0], root_recv.at[0], far_peer(far, far // 2)[1])
    exchange.start()
    own_rows = pl.ds(pl.multiple_of(spot * leaf, leaf), leaf)
    answer[own_rows] = take_out_targets(levels - 1, own_rows)
    take_out(levels - 1, own_rows, levels - 1)
    exchange.wait()
    inner = root_own[:, :order] + root_landed[:, :order]
    choose_cap(inner, lax.rem(device, 2**levels) == 2 ** (levels - 1))
    row = lax.broadcasted_iota(jnp.int32, (order, order), 0)
    lane = lax.broadcasted_iota(jnp.int32, (order, order), 1)
    cap[...] = cap[...] + jnp.where(row == lane, 1.0, 0.0)
    newton_start(levels, inner, rest, guess)
    gauss_jordan(cap, spread, logs, beside=functools.partial(newton_round, rest, guess, 0, 0))
    right = root_own[:, order:] + root_landed[:, order:]
    target_coef[...] = three_dot(halves(guess[...]), halves(right))
    own_answer = take_out_targets(levels, own_rows)
    answer_out[...] = own_answer[:, : answer_out.shape[1]]

    landed, passed, terms, own, near_send, near_recv, far_send, far_recv = last
    fits = jnp.sum(targets_ref[...] * own_answer, axis=0, keepdims=True)
    line = lax.broadcasted_iota(jnp.int32, terms.shape, 0)
    terms[...] = jnp.where(line == 0, fits, jnp.where(line == 1, logs[...] + log_ref[...], 0.0))
    here = near_peer(near, 0)[0]
    copies = []
    for k in range(1, near):
        device = near_peer(near, k)[2]
        copies.append(remote(terms, landed.at[here], near_send.at[k - 1], near_recv.at[k - 1], device))
        copies[-1].start()
    landed[here] = terms[...]
    for copy in copies:
        copy.wait()
    total = landed[0]
    for k in range(1, near):
        total = total + landed[k]
    own[...] = total
    index = far_peer(far, 0)[0]
    copies = []
    for k in range(1, far):
        copies.append(remote(own, passed.at[index], far_send.at[k - 1], far_recv.at[k - 1], far_peer(far, k)[1]))
        copies[-1].start()
    passed[index] = total
    for copy in copies:
        copy.wait()
    total = passed[0]
    for k in range(1, far):
        total = total + passed[k]
    share = 1.0 / (leaf * lax.axis_size("narrow") * lax.axis_size("wide"))
    fit_out[...] = total[0:1, : fit_out.shape[1]] * share
    logdet_out[...] = total[1:2, 0:1] * share


def tree(points, targets, noise, index, scales, rhs):
    leaf, feature = points.shape
    levels, order = scales.shape[0], index.shape[0] * 4 // 9
    points_in_line = LINE * leaf
    width = levels * order + LANES
    near, far = near_far(levels)
    dma = pltpu.SemaphoreType.DMA
    terms = (8, LANES)
    scratch = [
        VMEM((points_in_line, levels * order), jnp.bfloat16),
        VMEM((points_in_line, LANES), jnp.float32),
        VMEM((order, levels * order), jnp.bfloat16),
        VMEM((order, LANES), jnp.float32),
        VMEM((order, width + order + LANES), jnp.bfloat16),
        VMEM((order, points_in_line), jnp.bfloat16),
        VMEM((order, order), jnp.float32),
        VMEM((order, order), jnp.float32),
        VMEM((order, order), jnp.float32),
        VMEM((8, 8, LANES), jnp.float32),
        VMEM((1, LANES), jnp.float32),
        VMEM((order, points_in_line), jnp.bfloat16),
        VMEM((near, *terms), jnp.float32),
        VMEM((far, *terms), jnp.float32),
        VMEM(terms, jnp.float32),
        VMEM(terms, jnp.float32),
        *[dma((count - 1,)) for count in (near, near, far, far)],
    ]
    scratch += [VMEM((order, order + LANES), jnp.float32)] * 2 + [dma((1,))] * 2
    scratch += [
        VMEM((LINE, leaf, LANES), jnp.float32),
        VMEM((LINE, order, order), jnp.float32),
        VMEM((points_in_line, order), jnp.float32),
        VMEM((points_in_line, (levels - 1) * order), jnp.float32),
        VMEM((1, LANES), jnp.float32),
        *prologue_shapes(leaf, feature, order),
    ]
    for level in range(3, levels):
        extra = order + LANES if level == levels - 1 else 0
        scratch += level_shapes(level, order, width - (level - 1) * order + extra)
    return pl.pallas_call(
        functools.partial(tree_kernel, levels),
        out_shape=tuple(jax.ShapeDtypeStruct(shape, jnp.float32) for shape in ((leaf, rhs), (1, rhs), (1, 1))),
        in_specs=[*[pl.BlockSpec(memory_space=VMEM)] * 4, pl.BlockSpec(memory_space=pltpu.SMEM)],
        out_specs=(pl.BlockSpec(memory_space=VMEM),) * 3,
        scratch_shapes=scratch,
        compiler_params=pltpu.CompilerParams(
            collective_id=2, has_side_effects=True, vmem_limit_bytes=56 * 2**20
        ),
        name="tree",
    )(points, targets, noise, index, scales)


def per_device(embeddings, noise, targets, level_scale, skeleton):
    leaf, _ = embeddings.shape
    levels, _, rank = skeleton.shape
    rhs = targets.shape[1]
    wide_size = lax.axis_size("wide")
    device = lax.axis_index("narrow") * wide_size + lax.axis_index("wide")
    spot = lax.rem(device, LINE)
    quarter = rank // LINE
    scales = jnp.sqrt(level_scale / rank)
    local = skeleton[:, 0, :] - (device - spot) * leaf
    padded = jnp.concatenate(
        [targets, local[0].astype(jnp.float32)[:, None], jnp.zeros((leaf, LANES - rhs - 1), jnp.float32)], axis=1
    )
    own_rows = lax.dynamic_slice(local[2:], (0, spot * quarter), (levels - 2, quarter))
    index = jnp.concatenate([local[1], own_rows.reshape(-1)])[:, None]
    answer, fit, logdet = tree(embeddings, padded, noise[None, :], index, scales, rhs)
    return (answer, fit.reshape(rhs), logdet.reshape(()))


def solution(mesh):
    return jax.shard_map(
        per_device,
        mesh=mesh,
        in_specs=(
            P(NARROW_WIDE, None),
            P(NARROW_WIDE),
            P(NARROW_WIDE, None),
            P(),
            P(None, NARROW_WIDE, None),
        ),
        out_specs=(P(NARROW_WIDE, None), P(), P()),
        check_vma=False,
    )
```
